128 devices in a mesh: gx: 8 (over z, core), gy: 4 (over y), gz: 4 (over x).
Axes of the slice: x: 4, y: 4, z: 4, core: 2. Of those that a mesh axis runs over, the one named last changes fastest.
Arguments:
- pressure_rhs: float32 [128, 128, 2048], P('gx', 'gy', 'gz'), may hold values from -6 to 6
- shift_diag: float32 [128, 128, 2048], P('gx', 'gy', 'gz'), may hold values from 0.02 to 0.3
- positions: float32 [3, 1048576], P(None, ('gx', 'gy', 'gz')), may hold values from -6 to 6
- normals: float32 [3, 1048576], P(None, ('gx', 'gy', 'gz')), may hold values from -6 to 6
- tension: float32 [1048576], P(('gx', 'gy', 'gz')), may hold values from 0.3 to 3
- edge_weight: float32 [6, 1048576], P(None, ('gx', 'gy', 'gz')), may hold values from 0.5 to 2
- owner_map: int32 [1048576, 1], P(('gx', 'gy', 'gz')), may hold values from 0 to 127; in each aligned block of 8192 rows (0 to 8191, 8192 to 16383, ...) at most 256 rows name the same one
- cell_map: int32 [1048576], P(('gx', 'gy', 'gz')), may hold values from 0 to 262143
- connectivity: int32 [6, 1048576], P(None, ('gx', 'gy', 'gz')), may hold values from 0 to 1048575, as said below
Outputs:
- pressure: float32 [128, 128, 2048], P('gx', 'gy', 'gz')
- surface_force: float32 [3, 1048576], P(None, ('gx', 'gy', 'gz'))
The draws below stay inside these ranges and needn't reach their ends.
Inputs may be any that keep to these rules, and one draw needn't show every extreme that they name: `connectivity`: each neighbour index differs from the point's own index by 1 to 64, counted cyclically over 1048576; the distance 64 occurs. `owner_map`: among the points of one device no owner is named more than 256 times, a bound that some block reaches.
All inputs are finite; a program needn't handle non-finite values.
Results may differ from the reference program's by a relative error of at most 0.0003.
Values sent between devices are 32-bit elements; how exact they have to be, the bound alone decides.
No kernel may reach another device: no remote copies, remote signals or barrier semaphores. Data moves between devices by JAX's collectives and lax.ppermute only.
A program may use at most 192 MiB of HBM per device.

```python
import math
import jax
import jax.numpy as jnp
import numpy as np

CX = 16
CY = 32
CZ = 512
PTS_DEV = 8192
NEIGH = 6
HALO = 64
SMOOTH = 3
COARSE_SMOOTH = 4
POINTS = 1048576
CAP = 256
NX = 128
NY = 128
NZ = 2048
N_GY = 4
N_GZ = 4
DEVICES = 128


def draw_connectivity(key, part):
    first = jax.random.fold_in(key, 11)
    second = jax.random.fold_in(key, 12)
    reach = jax.random.randint(first, (NEIGH, POINTS), 1, HALO + 1)
    reach = reach.at[0, 0].set(HALO)
    sign = jax.random.randint(second, (NEIGH, POINTS), 0, 2) * 2 - 1
    base = jnp.arange(POINTS, dtype=jnp.int32)[None, :]
    return ((base + sign * reach) % POINTS).astype(jnp.int32)


def plant(entries, stream_key, smallest, high):
    dims = entries.shape
    place = [jax.random.randint(jax.random.fold_in(stream_key, axis), (), 0, dims[axis]) for axis in range(len(dims))]
    entries = entries.at[tuple(place)].set(smallest)
    longest = dims.index(max(dims))
    place[longest] = (place[longest] + 1) % dims[longest]
    return entries.at[tuple(place)].set(high)


def block_levels(own_key, extent, pieces, least, top_value):
    factor_of, own = 1.0, jax.random.fold_in(own_key, 6)
    for axis_at, shards_of in pieces:
        heights = jnp.exp(jax.random.uniform(jax.random.fold_in(own, axis_at), (shards_of,), jnp.float32, least / len(pieces), top_value / len(pieces)))
        factor_of = factor_of * jnp.repeat(heights, extent[axis_at] // shards_of).reshape([-1 if axis == axis_at else 1 for axis in range(len(extent))])
    return factor_of


def deal_out(key, own, number, rows, amount, top, most, slope):
    sequence = jax.random.permutation(key, amount)
    heavy_load, common = shares(amount, rows * top, most, slope, True), shares(amount, rows * top, most, slope, False)
    places = jnp.arange(amount)

    def named(tallies, rotation):
        used = int((tallies > 0).sum())
        fixed = max(1, used // 4)
        shifted = fixed + (places - fixed + rotation * (used - fixed)) % max(1, amount - fixed)
        return jnp.zeros((amount,), jnp.int32).at[sequence[jnp.where(places < fixed, places, shifted)]].set(jnp.asarray(tallies, jnp.int32))

    tallies = jnp.where(number % 4 == 0, named(heavy_load, number // 4), named(common, number - number // 4 - 1))
    mixed = jax.random.permutation(jax.random.fold_in(own, 3), amount)
    giver, taker = mixed[0:amount // 2 * 2:2], mixed[1:amount // 2 * 2:2]
    room = jnp.minimum(tallies[giver] - 1, most - tallies[taker]) // 2
    room = jnp.where((giver == sequence[0]) | (taker == sequence[0]) | (tallies[taker] == 0), 0, jnp.maximum(room, 0))
    shifted = jax.random.randint(jax.random.fold_in(own, 4), (amount // 2,), 0, 1 << 20) % (room + 1)
    tallies = tallies.at[giver].add(-shifted).at[taker].add(shifted)
    members = jnp.searchsorted(jnp.cumsum(tallies), jnp.arange(rows * top), side="right").astype(jnp.int32)
    listing = members.reshape(top, rows).T
    listing = listing[jax.random.permutation(jax.random.fold_in(own, 1), rows)]
    rotation = jax.random.randint(jax.random.fold_in(own, 2), (rows, 1), 0, top)
    return jnp.take_along_axis(listing, (jnp.arange(top)[None, :] + rotation) % top, axis=1)


def shares(count, total, bound, slope, full):
    weights = [(1 << 20) // math.isqrt(grade ** slope) + 1 for grade in range(1, count + 1)]
    largest = bound if full else min(bound, max(-(-total // count), total * weights[0] // sum(weights)))
    least = 1 if total - largest >= count - 1 else 0
    given, surplus = [largest] + [least] * (count - 1), total - largest - least * (count - 1)
    while surplus > 0:
        free = [i for i in range(1, count) if given[i] < largest] or [i for i in range(1, count) if given[i] < bound]
        whole, budget = sum([weights[i] for i in free]), surplus
        for i in free:
            more = min(bound - given[i], max(1, budget * weights[i] // whole), surplus)
            given[i] = given[i] + more
            surplus = surplus - more
    return np.array(given)


def scatter_about(stream_key, extent, scale, most, split=(), kind=jnp.bfloat16):
    gain = block_levels(stream_key, extent, split, -0.22, 0.18) if split else 1.0
    array = jax.random.normal(stream_key, extent, jnp.float32) * scale * gain
    return jnp.minimum(jnp.maximum(array, -most), most).astype(kind)


def setup_inputs(seed: int = 0) -> dict:
    keys = jax.random.split(jax.random.key(seed), 10)
    pressure_rhs = scatter_about(keys[0], (NX, NY, NZ), 1.0, 6.0, ((0, 8), (1, 4), (2, 4)), jnp.float32)
    shift_diag = jnp.clip(jnp.exp(math.log(0.3) - 2.7080503 * jax.random.uniform(keys[1], (NX, NY, NZ), jnp.float32) ** block_levels(keys[1], (NX, NY, NZ), ((0, 8), (1, 4), (2, 4)), -0.2, 0.2)), 0.02, 0.3)
    positions = scatter_about(keys[2], (3, POINTS), 1.0, 6.0, ((1, 128),), jnp.float32)
    normals = scatter_about(keys[3], (3, POINTS), 1.0, 6.0, ((1, 128),), jnp.float32)
    tension = jnp.clip(jnp.exp(math.log(3.0) - 2.3025851 * jax.random.uniform(keys[4], (POINTS,), jnp.float32) ** block_levels(keys[4], (POINTS,), ((0, 128),), -0.2, 0.2)), 0.3, 3.0)
    edge_weight = jnp.clip(jnp.exp(math.log(2.0) - 1.3862944 * jax.random.uniform(keys[5], (NEIGH, POINTS), jnp.float32) ** block_levels(keys[5], (NEIGH, POINTS), ((1, 128),), -0.2, 0.2)), 0.5, 2.0)
    owner_map_keys = jax.random.split(jax.random.fold_in(keys[6], 1), POINTS // PTS_DEV)
    owner_map_turns = jax.random.permutation(jax.random.fold_in(keys[6], 3), POINTS // PTS_DEV)
    owner_map = jax.vmap(lambda own, number: deal_out(jax.random.fold_in(keys[6], 2), own, number, PTS_DEV, DEVICES, 1, CAP, 2))(owner_map_keys, owner_map_turns).reshape((POINTS, 1))
    cell_map = plant(jax.random.randint(keys[7], (POINTS,), 0, CX * CY * CZ), jax.random.fold_in(keys[7], 1), 0, (CX * CY * CZ) - 1).astype(jnp.int32)
    connectivity = draw_connectivity(jax.random.fold_in(keys[9], 71), 0)
    return dict(pressure_rhs=pressure_rhs, shift_diag=shift_diag, positions=positions, normals=normals, tension=tension, edge_weight=edge_weight, owner_map=owner_map, cell_map=cell_map, connectivity=connectivity)


centre = 1.125
spread = 0.875


def operate(field, shift):
    padded = jnp.pad(field, 1)
    beside = padded[2:, 1:-1, 1:-1] + padded[:-2, 1:-1, 1:-1]
    beside = beside + padded[1:-1, 2:, 1:-1] + padded[1:-1, :-2, 1:-1]
    beside = beside + padded[1:-1, 1:-1, 2:] + padded[1:-1, 1:-1, :-2]
    return (6.0 + shift) * field - beside


def chebyshev(target, shift, start, sweeps):
    inverse = 1.0 / (6.0 + shift)
    ratio = centre / spread
    factor = 1.0 / ratio
    if start is None:
        update = inverse * target / centre
        answer = update
    else:
        update = inverse * (target - operate(start, shift)) / centre
        answer = start + update
    for sweep in range(1, sweeps):
        remain = inverse * (target - operate(answer, shift))
        factor_new = 1.0 / (2.0 * ratio - factor)
        update = factor_new * factor * update + (2.0 * factor_new / spread) * remain
        answer = answer + update
        factor = factor_new
    return answer


def blocks(field):
    nxh, nyh, nzh = field.shape[0] // 2, field.shape[1] // 2, field.shape[2] // 2
    return field.reshape(nxh, 2, nyh, 2, nzh, 2)


def reference(pressure_rhs, shift_diag, positions, normals, tension, edge_weight, owner_map, cell_map, connectivity):
    neighbours = positions[:, connectivity]
    surface_force = tension[None, :] * jnp.sum(edge_weight[None, :, :] * (neighbours - positions[:, None, :]), axis=1)
    jump = jnp.sum(surface_force * normals, axis=0)
    owner = owner_map[:, 0]
    ox = owner // (N_GY * N_GZ)
    oy = (owner // N_GZ) % N_GY
    oz = owner % N_GZ
    cx = cell_map // (CY * CZ)
    cy = (cell_map // CZ) % CY
    cz = cell_map % CZ
    forcing = pressure_rhs.at[ox * CX + cx, oy * CY + cy, oz * CZ + cz].add(jump)
    smooth = chebyshev(forcing, shift_diag, None, SMOOTH)
    remain = forcing - operate(smooth, shift_diag)
    coarse_rhs = 0.5 * jnp.sum(blocks(remain), axis=(1, 3, 5))
    coarse_shift = 4.0 * jnp.mean(blocks(shift_diag), axis=(1, 3, 5))
    coarse_fix = chebyshev(coarse_rhs, coarse_shift, None, COARSE_SMOOTH)
    spreadout = jnp.repeat(jnp.repeat(jnp.repeat(coarse_fix, 2, axis=0), 2, axis=1), 2, axis=2)
    pressure = chebyshev(forcing, shift_diag, smooth + spreadout, SMOOTH)
    return pressure, surface_force
```

```python
import jax
import jax.numpy as jnp
from jax import lax
from jax.experimental import pallas as pl
from jax.experimental.pallas import tpu as pltpu
from jax.sharding import PartitionSpec as P

CX, CY, CZ = 16, 32, 512
W = 5
EX = CX + 2 * W
EY = CY + 16
EZ = CZ + 128
ZB = -(-EX * EY // 128)
ALL = ("gx", "gy", "gz")
NPOINT = 8192
CAP = 256
NDEV = 128

CENTRE = 1.125
SPREAD = 0.875
RATIO = CENTRE / SPREAD


def factors(sweeps):
    factor, out = 1.0 / RATIO, []
    for _ in range(1, sweeps):
        fresh = 1.0 / (2.0 * RATIO - factor)
        out.append((fresh * factor, 2.0 * fresh / SPREAD))
        factor = fresh
    return out


def call(kernel, outs, operands, scratch=(), name=None, limit=40):
    specs = [
        pl.BlockSpec(memory_space=pltpu.SMEM)
        if o.dtype == jnp.int32 and o.ndim == 1
        else pl.BlockSpec(memory_space=pltpu.VMEM)
        for o in operands
    ]
    return pl.pallas_call(
        kernel,
        out_shape=[jax.ShapeDtypeStruct(s, jnp.float32) for s in outs],
        in_specs=specs,
        out_specs=[pl.BlockSpec(memory_space=pltpu.VMEM) for _ in outs],
        scratch_shapes=list(scratch),
        compiler_params=pltpu.CompilerParams(vmem_limit_bytes=limit << 20),
        name=name,
    )(*operands)


def lanes(shape):
    return lax.broadcasted_iota(jnp.int32, shape, len(shape) - 1)


def rows(shape):
    return lax.broadcasted_iota(jnp.int32, shape, len(shape) - 2)


def x_faces(force_ref, inv_ref, up_ref, low_ref, to_low_ref, to_up_ref):
    for which, ref in ((0, force_ref), (1, inv_ref)):
        for out, first in ((to_low_ref, 0), (to_up_ref, CX - W)):
            out[which, :, 0:CY, :] = ref[first : first + W]
            out[which, :, CY : CY + 8, :] = up_ref[which, first : first + W]
            out[which, :, CY + 8 : CY + 16, :] = low_ref[which, first : first + W]


def assemble(force_ref, inv_ref, yup_ref, ylow_ref, xup_ref, xlow_ref, f_ref, v_ref, to_low_ref, to_up_ref):
    for which, (src, dst) in enumerate(((force_ref, f_ref), (inv_ref, v_ref))):
        dst[0:W, :, 0:CZ] = xlow_ref[which]
        dst[W + CX :, :, 0:CZ] = xup_ref[which]
        dst[W : W + CX, 0:CY, 0:CZ] = src[...]
        dst[W : W + CX, CY : CY + 8, 0:CZ] = yup_ref[which]
        dst[W : W + CX, CY + 8 : CY + 16, 0:CZ] = ylow_ref[which]
    spot = lanes((128, 128))
    for j in range(ZB):
        first = min(128 * j, EX * EY - 128)

        def edge(ref, at):
            flat = ref.reshape(EX * EY, EZ)
            return flat[first : first + 128, at : at + 128]

        mixed = jnp.where(
            spot < 16,
            edge(f_ref, 0),
            jnp.where(
                spot < 32,
                pltpu.roll(edge(v_ref, 0), 16, 1),
                jnp.where(
                    spot < 48,
                    pltpu.roll(edge(f_ref, CZ - 128), 48, 1),
                    pltpu.roll(edge(v_ref, CZ - 128), 64, 1),
                ),
            ),
        )
        turned = mixed.T
        to_low_ref[:, 128 * j : 128 * j + 128] = turned[0:32]
        to_up_ref[:, 128 * j : 128 * j + 128] = turned[32:64]


def neighbours(ref, x, step):
    plane = ref[x]
    ny, nz = plane.shape
    beside = ref[x - 1] + ref[x + 1]
    beside = beside + (pltpu.roll(plane, 1, 0) + pltpu.roll(plane, ny - 1, 0))
    return plane, beside + (pltpu.roll(plane, step, 1) + pltpu.roll(plane, nz - step, 1))


def planes(first, last, body):
    def step(x, carry):
        body(x)
        return carry

    lax.fori_loop(first, last, step, 0)


def smooth_kernel(fin_ref, vin_ref, zup_ref, zlow_ref, f_ref, v_ref, a_ref, to_low_ref, to_up_ref, coarse_ref, b_ref, tmp_ref):
    f_ref[:, :, 0:CZ] = fin_ref[:, :, 0:CZ]
    v_ref[:, :, 0:CZ] = vin_ref[:, :, 0:CZ]
    gap = jnp.zeros((96, 128), jnp.float32)
    for j in range(ZB):
        first = min(128 * j, EX * EY - 128)
        at = slice(128 * j, 128 * j + 128)
        for dst, part in ((f_ref, slice(0, 16)), (v_ref, slice(16, 32))):
            stack = jnp.concatenate([zup_ref[part, at], gap, zlow_ref[part, at]], axis=0)
            dst.reshape(EX * EY, EZ)[first : first + 128, CZ:] = stack.T
    scale = 1.0 / CENTRE

    def start(x):
        a_ref[x] = v_ref[x] * f_ref[x] * scale

    planes(0, EX, start)
    (a1, b1), (a2, b2) = factors(3)

    def second(x):
        plane, beside = neighbours(a_ref, x, 1)
        left = v_ref[x] * (f_ref[x] + beside) - plane
        b_ref[x] = (1.0 + a1) * plane + b1 * left

    planes(1, EX - 1, second)

    def third(x):
        plane, beside = neighbours(b_ref, x, 1)
        left = v_ref[x] * (f_ref[x] + beside) - plane
        a_ref[x] = plane + a2 * (plane - a_ref[x]) + b2 * left

    planes(2, EX - 2, third)

    def restrict(xc, carry):
        total = jnp.zeros((CY, EZ), jnp.float32)
        weight = jnp.zeros((CY, EZ), jnp.float32)
        for half in range(2):
            x = W + 2 * xc + half
            plane, beside = neighbours(a_ref, x, 1)
            inv = v_ref[x, 0:CY]
            diag = jnp.where(inv > 0.0, 1.0 / inv, 0.0)
            total = total + ((f_ref[x] + beside)[0:CY] - diag * plane[0:CY])
            weight = weight + diag
        even = lanes((CY // 2, EZ)) % 2 == 0

        def pairs(value):
            value = value + pltpu.roll(value, EZ - 1, 1)
            parts = []
            for t in range(EZ // 128):
                tmp_ref[t] = value[:, 128 * t : 128 * t + 128]
                parts.append(tmp_ref[t, pl.ds(0, CY // 2, 2)] + tmp_ref[t, pl.ds(1, CY // 2, 2)])
            return jnp.concatenate(parts, axis=1)

        rhs = 0.5 * pairs(total)
        whole = pairs(weight)
        inv = jnp.where(whole > 0.0, 1.0 / (6.0 + 0.5 * (whole - 48.0)), 0.0)
        both = jnp.where(even, rhs, pltpu.roll(inv, 1, 1))
        coarse_ref[xc] = both
        to_low_ref[xc] = both[0:8]
        to_up_ref[xc] = both[8:16]
        return carry

    lax.fori_loop(0, CX // 2, restrict, 0)


def coarse_faces(own_ref, up_ref, low_ref, to_low_ref, to_up_ref):
    for out, first in ((to_low_ref, 0), (to_up_ref, CX // 2 - W)):
        out[:, 0:16] = own_ref[first : first + W]
        out[:, 16:24] = up_ref[first : first + W]
        out[:, 24:32] = low_ref[first : first + W]


def final_kernel(f_ref, v_ref, ain_ref, own_ref, yup_ref, ylow_ref, xup_ref, xlow_ref, out_ref, a_ref, b_ref, cb_ref, cv_ref, ca_ref, cc_ref, tmp_ref):
    even = lanes((32, EZ)) % 2 == 0

    def unpack(x, value):
        cb_ref[x] = jnp.where(even, value, pltpu.roll(value, 1, 1))
        cv_ref[x] = jnp.where(even, pltpu.roll(value, EZ - 1, 1), value)

    for x in range(W):
        unpack(x, xlow_ref[x])
        unpack(x + W + CX // 2, xup_ref[x])
    for x in range(CX // 2):
        unpack(x + W, jnp.concatenate([own_ref[x], yup_ref[x], ylow_ref[x]], axis=0))
    (a1, b1), (a2, b2), (a3, b3) = factors(4)
    scale = 1.0 / CENTRE
    ex = CX // 2 + 2 * W

    def start(x):
        ca_ref[x] = cv_ref[x] * cb_ref[x] * scale

    planes(0, ex, start)

    def sweep(src, dst, first, last, a, b, fresh):
        def body(x):
            plane, beside = neighbours(src, x, 2)
            left = cv_ref[x] * (cb_ref[x] + beside) - plane
            step = plane if fresh else plane - dst[x]
            dst[x] = plane + a * step + b * left

        planes(first, last, body)

    sweep(ca_ref, cc_ref, 1, ex - 1, a1, b1, True)
    sweep(cc_ref, ca_ref, 2, ex - 2, a2, b2, False)
    sweep(ca_ref, cc_ref, 3, ex - 3, a3, b3, False)

    def spread(x):
        coarse = cc_ref[(x + W) // 2]
        for t in range(EZ // 128):
            at = slice(128 * t, 128 * t + 128)
            tmp_ref[t, pl.ds(0, 32, 2)] = coarse[:, at]
            tmp_ref[t, pl.ds(1, 32, 2)] = coarse[:, at]
            a_ref[x, 0:40, at] = ain_ref[x, 0:40, at] + tmp_ref[t, 0:40]
            a_ref[x, 40:48, at] = ain_ref[x, 40:48, at] + tmp_ref[t, 56:64]

    planes(2, EX - 2, spread)
    (a1, b1), (a2, b2) = factors(3)

    def first(x):
        plane, beside = neighbours(a_ref, x, 1)
        left = v_ref[x] * (f_ref[x] + beside) - plane
        b_ref[x] = plane + scale * left

    planes(3, EX - 3, first)

    def second(x):
        plane, beside = neighbours(b_ref, x, 1)
        left = v_ref[x] * (f_ref[x] + beside) - plane
        a_ref[x] = plane + a1 * (plane - a_ref[x]) + b1 * left

    planes(4, EX - 4, second)

    def third(x):
        plane, beside = neighbours(a_ref, x, 1)
        left = v_ref[x] * (f_ref[x] + beside) - plane
        full = plane + a2 * (plane - b_ref[x]) + b2 * left
        out_ref[x - W] = full[0:CY, 0:CZ]

    planes(W, W + CX, third)


def swap(low, high, axis):
    count = lax.axis_size(axis)
    up = [(i, i + 1) for i in range(count - 1)]
    return lax.ppermute(low, axis, [(b, a) for a, b in up]), lax.ppermute(high, axis, up)


def solve(forcing, inverse, to_low, to_up):
    yup, ylow = swap(to_low, to_up, "gy")
    face = (2, W, EY, CZ)
    xs = call(x_faces, [face, face], (forcing, inverse, yup, ylow), name="x_faces")
    xup, xlow = swap(*xs, "gx")
    ext = (EX, EY, EZ)
    f, v, zl, zu = call(
        assemble,
        [ext, ext, (32, 128 * ZB), (32, 128 * ZB)],
        (forcing, inverse, yup, ylow, xup, xlow),
        name="assemble",
    )
    zup, zlow = swap(zl, zu, "gz")
    cy, cx = (CX // 2, 8, EZ), (W, 32, EZ)
    f, v, a, yl, yu, own = call(
        smooth_kernel,
        [ext, ext, ext, cy, cy, (CX // 2, CY // 2, EZ)],
        (f, v, zup, zlow),
        [pltpu.VMEM(ext, jnp.float32), pltpu.VMEM((EZ // 128, CY, 128), jnp.float32)],
        name="smooth",
    )
    yup, ylow = swap(yl, yu, "gy")
    xs = call(coarse_faces, [cx, cx], (own, yup, ylow), name="coarse_faces")
    xup, xlow = swap(*xs, "gx")
    cext = (CX // 2 + 2 * W, 32, EZ)
    return call(
        final_kernel,
        [(CX, CY, CZ)],
        (f, v, a, own, yup, ylow, xup, xlow),
        [pltpu.VMEM(ext, jnp.float32)] * 2
        + [pltpu.VMEM(cext, jnp.float32)] * 4
        + [pltpu.VMEM((EZ // 128, 64, 128), jnp.float32)],
        name="final",
        limit=50,
    )[0]


def points_kernel(begin_ref, pos_ref, low_ref, up_ref, nrm_ref, ten_ref, edge_ref, conn_ref, force_ref, jump_ref):
    half = lanes((1, 128)) < 64
    tiles = NPOINT // 128

    def tile(ref, row, t):
        if t < 0:
            return low_ref[row : row + 1, :]
        if t >= tiles:
            return up_ref[row : row + 1, :]
        return ref[row : row + 1, 128 * t : 128 * t + 128]

    for t in range(tiles):
        at = slice(128 * t, 128 * t + 128)
        conn = conn_ref[:, at]
        edge = edge_ref[:, at]
        tension = ten_ref[t : t + 1, :]
        same = (conn >> 7) == begin_ref[0] + t
        spot = conn & 127
        jump = jnp.zeros((1, 128), jnp.float32)
        for c in range(3):
            own = tile(pos_ref, c, t)
            other = jnp.where(half, tile(pos_ref, c, t + 1), tile(pos_ref, c, t - 1))
            shape = conn.shape
            near = jnp.take_along_axis(jnp.broadcast_to(own, shape), spot, axis=1, mode="promise_in_bounds")
            far = jnp.take_along_axis(jnp.broadcast_to(other, shape), spot, axis=1, mode="promise_in_bounds")
            pull = jnp.sum(edge * (jnp.where(same, near, far) - own), axis=0, keepdims=True)
            force = tension * pull
            force_ref[c : c + 1, at] = force
            jump = jump + force * nrm_ref[c : c + 1, at]
        jump_ref[t : t + 1, :] = jump


def slot_ranks(owner_ids, ndevice, npoint):
    block_len = 128
    nblock = npoint // block_len
    owner_hot = (owner_ids[:, None] == jnp.arange(ndevice, dtype=jnp.int32)[None, :]).astype(jnp.bfloat16)
    owner_blocks = owner_hot.reshape(nblock, block_len, ndevice)
    lower_tri = (jnp.arange(block_len)[:, None] > jnp.arange(block_len)[None, :]).astype(jnp.bfloat16)
    within = jnp.einsum("pq,bqo->bpo", lower_tri, owner_blocks, preferred_element_type=jnp.float32)
    counts = jnp.sum(owner_blocks.astype(jnp.float32), axis=1)
    before = jnp.cumsum(counts, axis=0) - counts
    ranks = jnp.sum((within + before[:, None, :]) * owner_blocks.astype(jnp.float32), axis=2)
    return (ranks.reshape(npoint).astype(jnp.int32), owner_hot)


def scatter_kernel(rhs_ref, shift_ref, got_ref, force_ref, inv_ref, to_low_ref, to_up_ref, acc_ref):
    group = 8
    acc_ref[...] = jnp.zeros((512, 512), jnp.float32)

    def step(g, carry):
        got = got_ref[pl.ds(g * group, group), :]
        left, right = [], []
        for i in range(group):
            value = got[i : i + 1, 0:CAP]
            cell = got[i : i + 1, CAP : 2 * CAP].astype(jnp.int32)
            top = value.astype(jnp.bfloat16).astype(jnp.float32)
            rest = value - top
            spot = lax.broadcasted_iota(jnp.int32, (512, CAP), 0)
            on_row = (cell >> 9) == spot
            on_col = jnp.where((cell & 511) == spot, 1.0, 0.0).astype(jnp.bfloat16)
            left += [jnp.where(on_row, top, 0.0).astype(jnp.bfloat16), jnp.where(on_row, rest, 0.0).astype(jnp.bfloat16)]
            right += [on_col, on_col]
        acc_ref[...] += lax.dot_general(
            jnp.concatenate(left, axis=1),
            jnp.concatenate(right, axis=1),
            (((1,), (1,)), ((), ())),
            preferred_element_type=jnp.float32,
        )
        return carry

    lax.fori_loop(0, NDEV // group, step, 0)

    def finish(x, carry):
        force = rhs_ref[x] + acc_ref[pl.ds(x * CY, CY), :]
        inv = 1.0 / (6.0 + shift_ref[x])
        force_ref[x] = force
        inv_ref[x] = inv
        for which, value in ((0, force), (1, inv)):
            to_low_ref[which, x] = value[0:8]
            to_up_ref[which, x] = value[CY - 8 : CY]
        return carry

    lax.fori_loop(0, CX, finish, 0)


def body(pressure_rhs, shift_diag, positions, normals, tension, edge_weight, owner_map, cell_map, connectivity):
    device = lax.axis_index(ALL)
    begin = (device * (NPOINT // 128)).reshape(1).astype(jnp.int32)
    ring = [(i, (i + 1) % NDEV) for i in range(NDEV)]
    low = lax.ppermute(positions[:, NPOINT - 128 :], ALL, ring)
    up = lax.ppermute(positions[:, :128], ALL, [(b, a) for a, b in ring])
    force, jump = call(
        points_kernel,
        [(3, NPOINT), (NPOINT // 128, 128)],
        (begin, positions, low, up, normals, tension.reshape(-1, 128), edge_weight, connectivity),
        name="points",
    )
    jump = jump.reshape(-1)
    ranks, owner_hot = slot_ranks(owner_map[:, 0], NDEV, NPOINT)
    rank_hot = (ranks[:, None] == jnp.arange(CAP, dtype=jnp.int32)[None, :]).astype(jnp.float32)
    carried = jnp.stack([jump, cell_map.astype(jnp.float32)], axis=0)
    weighted = carried[:, :, None] * rank_hot[None, :, :]
    packed = jnp.einsum("po,kpr->okr", owner_hot.astype(jnp.float32), weighted, precision=lax.Precision.HIGHEST)
    got = lax.all_to_all(packed.reshape(NDEV, 2 * CAP), ALL, 0, 0, tiled=True)
    block = (CX, CY, CZ)
    forcing, inverse, to_low, to_up = call(
        scatter_kernel,
        [block, block, (2, CX, 8, CZ), (2, CX, 8, CZ)],
        (pressure_rhs, shift_diag, got),
        [pltpu.VMEM((512, 512), jnp.float32)],
        name="scatter",
    )
    return solve(forcing, inverse, to_low, to_up), force


def solution(mesh):
    point, row = P(ALL), P(None, ALL)
    grid = P("gx", "gy", "gz")
    return jax.shard_map(
        body,
        mesh=mesh,
        in_specs=(grid, grid, row, row, point, row, P(ALL, None), point, row),
        out_specs=(grid, row),
        check_vma=False,
    )
```

```python
import jax
import jax.numpy as jnp
from jax import lax
from jax.experimental import pallas as pl
from jax.experimental.pallas import tpu as pltpu
from jax.sharding import PartitionSpec as P

CX, CY, CZ = 16, 32, 512
W = 5
EX = CX + 2 * W
EY = CY + 16
EZ = CZ + 128
ZB = -(-EX * EY // 128)
ALL = ("gx", "gy", "gz")
NPOINT = 8192
CAP = 256
NDEV = 128

CENTRE = 1.125
SPREAD = 0.875
RATIO = CENTRE / SPREAD


def factors(sweeps):
    factor, out = 1.0 / RATIO, []
    for _ in range(1, sweeps):
        fresh = 1.0 / (2.0 * RATIO - factor)
        out.append((fresh * factor, 2.0 * fresh / SPREAD))
        factor = fresh
    return out


def call(kernel, outs, operands, scratch=(), name=None, limit=4, alias=None):
    specs = [
        pl.BlockSpec(memory_space=pltpu.SMEM)
        if o.dtype == jnp.int32 and o.ndim == 1
        else pl.BlockSpec(memory_space=pltpu.VMEM)
        for o in operands
    ]
    return pl.pallas_call(
        kernel,
        out_shape=[jax.ShapeDtypeStruct(s, jnp.float32) for s in outs],
        in_specs=specs,
        out_specs=[pl.BlockSpec(memory_space=pltpu.VMEM) for _ in outs],
        scratch_shapes=list(scratch),
        compiler_params=pltpu.CompilerParams(vmem_limit_bytes=limit << 20),
        input_output_aliases=alias or {},
        name=name,
    )(*operands)


def lanes(shape):
    return lax.broadcasted_iota(jnp.int32, shape, len(shape) - 1)


def rows(shape):
    return lax.broadcasted_iota(jnp.int32, shape, len(shape) - 2)


def x_faces(force_ref, inv_ref, up_ref, low_ref, to_low_ref, to_up_ref):
    for which, ref in ((0, force_ref), (1, inv_ref)):
        for out, first in ((to_low_ref, 0), (to_up_ref, CX - W)):
            out[which, :, 0:CY, :] = ref[first : first + W]
            out[which, :, CY : CY + 8, :] = up_ref[which, first : first + W]
            out[which, :, CY + 8 : CY + 16, :] = low_ref[which, first : first + W]


def assemble(force_ref, inv_ref, yup_ref, ylow_ref, xup_ref, xlow_ref, f_ref, v_ref, to_low_ref, to_up_ref):
    for which, (src, dst) in enumerate(((force_ref, f_ref), (inv_ref, v_ref))):
        dst[0:W, :, 0:CZ] = xlow_ref[which]
        dst[W + CX :, :, 0:CZ] = xup_ref[which]
        dst[W : W + CX, 0:CY, 0:CZ] = src[...]
        dst[W : W + CX, CY : CY + 8, 0:CZ] = yup_ref[which]
        dst[W : W + CX, CY + 8 : CY + 16, 0:CZ] = ylow_ref[which]
    spot = lanes((128, 128))
    for j in range(ZB):
        first = min(128 * j, EX * EY - 128)

        def edge(ref, at):
            flat = ref.reshape(EX * EY, EZ)
            return flat[first : first + 128, at : at + 128]

        mixed = jnp.where(
            spot < 16,
            edge(f_ref, 0),
            jnp.where(
                spot < 32,
                pltpu.roll(edge(v_ref, 0), 16, 1),
                jnp.where(
                    spot < 48,
                    pltpu.roll(edge(f_ref, CZ - 128), 48, 1),
                    pltpu.roll(edge(v_ref, CZ - 128), 64, 1),
                ),
            ),
        )
        turned = mixed.T
        to_low_ref[:, 128 * j : 128 * j + 128] = turned[0:32]
        to_up_ref[:, 128 * j : 128 * j + 128] = turned[32:64]


def neighbours(ref, x, step):
    plane = ref[x]
    ny, nz = plane.shape
    beside = ref[x - 1] + ref[x + 1]
    beside = beside + (pltpu.roll(plane, 1, 0) + pltpu.roll(plane, ny - 1, 0))
    return plane, beside + (pltpu.roll(plane, step, 1) + pltpu.roll(plane, nz - step, 1))


def planes(first, last, body):
    def step(x, carry):
        body(x)
        return carry

    lax.fori_loop(first, last, step, 0)


def smooth_kernel(_fin_ref, _vin_ref, zup_ref, zlow_ref, f_ref, v_ref, a_ref, to_low_ref, to_up_ref, coarse_ref, b_ref, tmp_ref):
    gap = jnp.zeros((96, 128), jnp.float32)
    for j in range(ZB):
        first = min(128 * j, EX * EY - 128)
        at = slice(128 * j, 128 * j + 128)
        for dst, part in ((f_ref, slice(0, 16)), (v_ref, slice(16, 32))):
            stack = jnp.concatenate([zup_ref[part, at], gap, zlow_ref[part, at]], axis=0)
            dst.reshape(EX * EY, EZ)[first : first + 128, CZ:] = stack.T
    scale = 1.0 / CENTRE

    def start(x):
        a_ref[x] = v_ref[x] * f_ref[x] * scale

    planes(0, EX, start)
    (a1, b1), (a2, b2) = factors(3)

    def second(x):
        plane, beside = neighbours(a_ref, x, 1)
        left = v_ref[x] * (f_ref[x] + beside) - plane
        b_ref[x] = (1.0 + a1) * plane + b1 * left

    planes(1, EX - 1, second)

    def third(x):
        plane, beside = neighbours(b_ref, x, 1)
        left = v_ref[x] * (f_ref[x] + beside) - plane
        a_ref[x] = plane + a2 * (plane - a_ref[x]) + b2 * left

    planes(2, EX - 2, third)

    def restrict(xc, carry):
        total = jnp.zeros((CY, EZ), jnp.float32)
        weight = jnp.zeros((CY, EZ), jnp.float32)
        for half in range(2):
            x = W + 2 * xc + half
            plane, beside = neighbours(a_ref, x, 1)
            inv = v_ref[x, 0:CY]
            diag = jnp.where(inv > 0.0, 1.0 / inv, 0.0)
            total = total + ((f_ref[x] + beside)[0:CY] - diag * plane[0:CY])
            weight = weight + diag
        even = lanes((CY // 2, EZ)) % 2 == 0

        def pairs(value):
            value = value + pltpu.roll(value, EZ - 1, 1)
            parts = []
            for t in range(EZ // 128):
                tmp_ref[t] = value[:, 128 * t : 128 * t + 128]
                parts.append(tmp_ref[t, pl.ds(0, CY // 2, 2)] + tmp_ref[t, pl.ds(1, CY // 2, 2)])
            return jnp.concatenate(parts, axis=1)

        rhs = 0.5 * pairs(total)
        whole = pairs(weight)
        inv = jnp.where(whole > 0.0, 1.0 / (6.0 + 0.5 * (whole - 48.0)), 0.0)
        both = jnp.where(even, rhs, pltpu.roll(inv, 1, 1))
        coarse_ref[xc] = both
        to_low_ref[xc] = both[0:8]
        to_up_ref[xc] = both[8:16]
        return carry

    lax.fori_loop(0, CX // 2, restrict, 0)


def coarse_faces(own_ref, up_ref, low_ref, to_low_ref, to_up_ref):
    for out, first in ((to_low_ref, 0), (to_up_ref, CX // 2 - W)):
        out[:, 0:16] = own_ref[first : first + W]
        out[:, 16:24] = up_ref[first : first + W]
        out[:, 24:32] = low_ref[first : first + W]


def final_kernel(f_ref, v_ref, ain_ref, own_ref, yup_ref, ylow_ref, xup_ref, xlow_ref, out_ref, a_ref, b_ref, cb_ref, cv_ref, ca_ref, cc_ref, tmp_ref):
    even = lanes((32, EZ)) % 2 == 0

    def unpack(x, value):
        cb_ref[x] = jnp.where(even, value, pltpu.roll(value, 1, 1))
        cv_ref[x] = jnp.where(even, pltpu.roll(value, EZ - 1, 1), value)

    for x in range(W):
        unpack(x, xlow_ref[x])
        unpack(x + W + CX // 2, xup_ref[x])
    for x in range(CX // 2):
        unpack(x + W, jnp.concatenate([own_ref[x], yup_ref[x], ylow_ref[x]], axis=0))
    (a1, b1), (a2, b2), (a3, b3) = factors(4)
    scale = 1.0 / CENTRE
    ex = CX // 2 + 2 * W

    def start(x):
        ca_ref[x] = cv_ref[x] * cb_ref[x] * scale

    planes(0, ex, start)

    def sweep(src, dst, first, last, a, b, fresh):
        def body(x):
            plane, beside = neighbours(src, x, 2)
            left = cv_ref[x] * (cb_ref[x] + beside) - plane
            step = plane if fresh else plane - dst[x]
            dst[x] = plane + a * step + b * left

        planes(first, last, body)

    sweep(ca_ref, cc_ref, 1, ex - 1, a1, b1, True)
    sweep(cc_ref, ca_ref, 2, ex - 2, a2, b2, False)
    sweep(ca_ref, cc_ref, 3, ex - 3, a3, b3, False)

    def spread(x):
        coarse = cc_ref[(x + W) // 2]
        for t in range(EZ // 128):
            at = slice(128 * t, 128 * t + 128)
            tmp_ref[t, pl.ds(0, 32, 2)] = coarse[:, at]
            tmp_ref[t, pl.ds(1, 32, 2)] = coarse[:, at]
            a_ref[x, 0:40, at] = ain_ref[x, 0:40, at] + tmp_ref[t, 0:40]
            a_ref[x, 40:48, at] = ain_ref[x, 40:48, at] + tmp_ref[t, 56:64]

    planes(2, EX - 2, spread)
    (a1, b1), (a2, b2) = factors(3)

    def first(x):
        plane, beside = neighbours(a_ref, x, 1)
        left = v_ref[x] * (f_ref[x] + beside) - plane
        b_ref[x] = plane + scale * left

    planes(3, EX - 3, first)

    def second(x):
        plane, beside = neighbours(b_ref, x, 1)
        left = v_ref[x] * (f_ref[x] + beside) - plane
        a_ref[x] = plane + a1 * (plane - a_ref[x]) + b1 * left

    planes(4, EX - 4, second)

    def third(x):
        plane, beside = neighbours(a_ref, x, 1)
        left = v_ref[x] * (f_ref[x] + beside) - plane
        full = plane + a2 * (plane - b_ref[x]) + b2 * left
        out_ref[x - W] = full[0:CY, 0:CZ]

    planes(W, W + CX, third)


def swap(low, high, axis):
    count = lax.axis_size(axis)
    up = [(i, i + 1) for i in range(count - 1)]
    return lax.ppermute(low, axis, [(b, a) for a, b in up]), lax.ppermute(high, axis, up)


def solve(forcing, inverse, to_low, to_up):
    yup, ylow = swap(to_low, to_up, "gy")
    face = (2, W, EY, CZ)
    xs = call(x_faces, [face, face], (forcing, inverse, yup, ylow), name="x_faces")
    xup, xlow = swap(*xs, "gx")
    ext = (EX, EY, EZ)
    f, v, zl, zu = call(
        assemble,
        [ext, ext, (32, 128 * ZB), (32, 128 * ZB)],
        (forcing, inverse, yup, ylow, xup, xlow),
        name="assemble",
    )
    zup, zlow = swap(zl, zu, "gz")
    cy, cx = (CX // 2, 8, EZ), (W, 32, EZ)
    f, v, a, yl, yu, own = call(
        smooth_kernel,
        [ext, ext, ext, cy, cy, (CX // 2, CY // 2, EZ)],
        (f, v, zup, zlow),
        [pltpu.VMEM(ext, jnp.float32), pltpu.VMEM((EZ // 128, CY, 128), jnp.float32)],
        name="smooth",
        limit=8,
        alias={0: 0, 1: 1},
    )
    yup, ylow = swap(yl, yu, "gy")
    xs = call(coarse_faces, [cx, cx], (own, yup, ylow), name="coarse_faces")
    xup, xlow = swap(*xs, "gx")
    cext = (CX // 2 + 2 * W, 32, EZ)
    return call(
        final_kernel,
        [(CX, CY, CZ)],
        (f, v, a, own, yup, ylow, xup, xlow),
        [pltpu.VMEM(ext, jnp.float32)] * 2
        + [pltpu.VMEM(cext, jnp.float32)] * 4
        + [pltpu.VMEM((EZ // 128, 64, 128), jnp.float32)],
        name="final",
        limit=20,
    )[0]


def bit_of(b, nv):
    if b < 3:
        return (lax.broadcasted_iota(jnp.int32, (8, 128), 0) >> b) & 1
    return (lax.broadcasted_iota(jnp.int32, (8, 128), 1) >> (b - 3 - nv)) & 1


def in_list(b, nv):
    return 3 <= b < 3 + nv


def across(x, b, nv, high):
    axis, size, d = (0, 8, 1 << b) if b < 3 else (1, 128, 1 << (b - 3 - nv))
    if 2 * d == size:
        return pltpu.roll(x, d, axis)
    return jnp.where(high, pltpu.roll(x, d, axis), pltpu.roll(x, size - d, axis))


def exchange(keys, values, b, nv):
    if in_list(b, nv):
        d = 1 << (b - 3)
        for u in range(len(keys)):
            if u & d:
                continue
            low, high = keys[u], keys[u + d]
            turn = low > high
            keys[u], keys[u + d] = jnp.minimum(low, high), jnp.maximum(low, high)
            a, c = values[u], values[u + d]
            values[u], values[u + d] = jnp.where(turn, c, a), jnp.where(turn, a, c)
        return
    high = bit_of(b, nv) != 0
    others = [across(key, b, nv, high) for key in keys]
    loads = [across(value, b, nv, high) for value in values]
    for u, other in enumerate(others):
        key = keys[u]
        keys[u] = jnp.where(high, jnp.maximum(key, other), jnp.minimum(key, other))
        values[u] = jnp.where(keys[u] != key, loads[u], values[u])


SIGN = -(1 << 31)


def route(goal, loads, b, nv, g):
    mask, one = jnp.int32(SIGN | (1 << g)), 1 << g
    if in_list(b, nv):
        d = 1 << (b - 3)
        for u in range(len(goal)):
            if u & d:
                continue
            low, high = goal[u], goal[u + d]
            ml, mh = low & mask, high & mask
            stay_l, stay_h = ml == 0, mh == one
            goal[u] = jnp.where(stay_l, low, jnp.where(mh == 0, high, -1))
            goal[u + d] = jnp.where(stay_h, high, jnp.where(ml == one, low, -1))
            for load in loads:
                a, c = load[u], load[u + d]
                load[u], load[u + d] = jnp.where(stay_l, a, c), jnp.where(stay_h, c, a)
        return
    place = bit_of(b, nv)
    high = place != 0
    place = place << g
    others = [across(x, b, nv, high) for x in goal]
    moved = [[across(x, b, nv, high) for x in load] for load in loads]
    for u, other in enumerate(others):
        own = goal[u]
        stay = (own & mask) == place
        goal[u] = jnp.where(stay, own, jnp.where((other & mask) == place, other, -1))
        for load, move in zip(loads, moved):
            load[u] = jnp.where(stay, load[u], move[u])


NONE = 1 << 18


def pack(owner_ref, cell_ref, jump_ref, turn, out_ref, key_ref, val_ref, goal_ref):
    nv = 3
    keys, values = [], []
    for u in range(8):
        at = slice(8 * u, 8 * u + 8)
        cell = cell_ref[at, :]
        mixed = (
            ((cell >> 15) << 15)
            | ((cell & 127) << 8)
            | ((cell >> 14) & 1) << 7
            | ((cell >> 12) & 3) << 5
            | ((cell >> 7) & 3) << 3
            | (cell >> 9) & 7
        )
        mixed = mixed ^ (turn * (NONE - 1))
        keys.append((owner_ref[at, :] << 18) | mixed)
        values.append(jump_ref[at, :])
    for k in range(1, 14):

        def flip(keys):
            if k == 13:
                return keys
            if in_list(k, nv):
                return [~key if (u >> (k - 3)) & 1 else key for u, key in enumerate(keys)]
            turned = -bit_of(k, nv)
            return [key ^ turned for key in keys]

        keys = flip(keys)
        for b in range(k - 1, -1, -1):
            exchange(keys, values, b, nv)
        keys = flip(keys)
    owners = [key >> 18 for key in keys]
    spot = 64 * lanes((8, 128)) + rows((8, 128))
    tail = [(owner << 13) | (8 * u + spot) for u, owner in enumerate(owners)]
    runs = list(tail)
    for b in range(13):
        if in_list(b, nv):
            d = 1 << (b - 3)
            other = [tail[u ^ d] for u in range(8)]
        else:
            d, high = 0, bit_of(b, nv) != 0
            other = [across(x, b, nv, high) for x in tail]
        for u in range(8):
            same = (other[u] ^ tail[u]) < 8192
            joins = (other[u] ^ runs[u]) < 8192
            if not d:
                runs[u] = jnp.where(high & joins, other[u], runs[u])
                tail[u] = jnp.where(high == same, other[u], tail[u])
            elif u & d:
                runs[u] = jnp.where(joins, other[u], runs[u])
                tail[u] = jnp.where(same, other[u], tail[u])
            else:
                tail[u] = jnp.where(same, tail[u], other[u])
    for u in range(8):
        at = slice(8 * u, 8 * u + 8)
        goal_ref[at, :] = 256 * owners[u] + 8 * u + spot - (runs[u] & 8191)
        key_ref[at, :] = (keys[u] & (NONE - 1)) ^ (turn * (NONE - 1))
        val_ref[at, :] = values[u]
    empty = NONE * (1 - turn) - turn

    def block(q, carry):
        sets = []
        for i in range(2):
            goal, key, value = [], [], []
            for u in range(8):
                at = slice(8 * u, 8 * u + 8)
                g = goal_ref[at, :]
                goal.append(jnp.where((g >> 13) == 2 * q + i, g & 8191, -1))
                key.append(key_ref[at, :])
                value.append(val_ref[at, :])
            sets.append((goal, key, value))
        for b in range(12, -1, -1):
            for goal, key, value in sets:
                route(goal, [key, value], b, nv, b)
        for i, (goal, key, value) in enumerate(sets):
            full = [g >= 0 for g in goal]
            parts = [jnp.where(f, v, 0.0) for f, v in zip(full, value)]
            parts += [jnp.where(f, c, empty).astype(jnp.float32) for f, c in zip(full, key)]
            first = pl.multiple_of(256 * q + 128 * i, 128)
            out_ref[pl.ds(first, 128), :] = jnp.concatenate(parts, axis=0).T
        return carry

    lax.fori_loop(0, 2, block, 0)


def regs(ref, first, count, step=8):
    return [ref[pl.ds(first + step * u, 8), :] for u in range(count)]


def put(ref, first, parts, step=8):
    for u, part in enumerate(parts):
        ref[pl.ds(first + step * u, 8), :] = part


def shifted(x, d):
    if d >= 256:
        return pltpu.roll(x, d // 256, 1)
    y = pltpu.roll(x, d, 0)
    head = max(d, 8)
    edge = jnp.where(rows((head, 128)) < d, pltpu.roll(y[:head], 1, 1), y[:head])
    return jnp.concatenate([edge, y[head:]], axis=0) if head < 256 else edge


def unpack_and_merge(got_ref, key_ref, val_ref):
    nv = 5
    for quarter in range(4):
        turned = got_ref[pl.ds(quarter, 128, 4), :].T
        val_ref[64 * quarter : 64 * quarter + 64, :] = turned[:64]
        key_ref[64 * quarter : 64 * quarter + 64, :] = turned[64:].astype(jnp.int32)
    before = 0
    for k in range(9, 16):
        turned = -bit_of(k, nv) if k < 15 else 0
        change = turned ^ before
        before = turned
        for b in range(k - 1, 7, -1):
            for half in range(2):
                keys, values = regs(key_ref, 128 * half, 16), regs(val_ref, 128 * half, 16)
                if b == k - 1:
                    keys = [key ^ change for key in keys]
                exchange(keys, values, b, nv)
                put(key_ref, 128 * half, keys)
                put(val_ref, 128 * half, values)
        for u in range(8):
            keys, values = regs(key_ref, 8 * u, 4, 64), regs(val_ref, 8 * u, 4, 64)
            for b in (4, 3):
                exchange(keys, values, b, 2)
            put(key_ref, 8 * u, keys, 64)
            put(val_ref, 8 * u, values, 64)
        for u in range(4):
            keys, values = regs(key_ref, 64 * u, 8), regs(val_ref, 64 * u, 8)
            for b in range(5, -1, -1):
                exchange(keys, values, b, 3)
            put(key_ref, 64 * u, keys)
            put(val_ref, 64 * u, values)


def combine(key_ref, val_ref, rank_ref):
    spot = rows((256, 128)) + 256 * lanes((256, 128))

    def gather(d):
        key, value = key_ref[...], val_ref[...]
        same = (shifted(key, d) == key) & (spot >= d)
        val_ref[...] = value + jnp.where(same, shifted(value, d), 0.0)

    for d in (1, 2, 4):
        gather(d)
    key = key_ref[...]
    real = (key >= 0) & (key < NONE)
    long = jnp.where(real & (shifted(key, 8) == key) & (spot >= 8), 1.0, 0.0)

    @pl.when(jnp.max(long) > 0.0)
    def _():
        for e in range(3, 15):
            gather(1 << e)

    after = pltpu.roll(key, 255, 0)
    edge = jnp.where(rows((8, 128)) == 7, pltpu.roll(after[248:], 127, 1), after[248:])
    after = jnp.concatenate([after[:248], edge], axis=0)
    last = real & ((after != key) | (spot == 32767))
    one = lambda test: jnp.where(test, 1.0, 0.0).astype(jnp.bfloat16)
    mask = one(last)
    dot = lambda a, b: jnp.dot(a, b, preferred_element_type=jnp.float32)
    within = dot(one(rows((256, 256)) > lanes((256, 256))), mask)
    totals = dot(jnp.ones((256, 256), jnp.bfloat16), mask).astype(jnp.bfloat16)
    before = dot(totals, one(rows((128, 128)) < lanes((128, 128))))
    rank_ref[...] = jnp.where(last, (within + before).astype(jnp.int32), -1)


def concentrate(key_ref, val_ref, rank_ref, turn_key_ref, turn_val_ref):
    refs = (rank_ref, key_ref, val_ref)

    def stages(first, count, step, bits):
        goal, key, value = (regs(r, first, count, step) for r in refs)
        for b, nv, g in bits:
            route(goal, [key, value], b, nv, g)
        for r, parts in zip(refs, (goal, key, value)):
            put(r, first, parts, step)

    for u in range(4):
        stages(64 * u, 8, 8, [(b, 3, b) for b in range(6)])
    for u in range(8):
        stages(8 * u, 4, 64, [(3, 2, 6), (4, 2, 7)])
    for b in range(8, 15):
        for half in range(2):
            stages(128 * half, 16, 8, [(b, 5, b)])
    for half in range(2):
        at = slice(128 * half, 128 * half + 128)
        turn_key_ref[at, :] = jnp.where(rank_ref[at, :] >= 0, key_ref[at, :], -1).T
        turn_val_ref[at, :] = val_ref[at, :].T


def distribute(turn_key_ref, turn_val_ref, goal_ref, move_ref, write):
    def block(q, carry):
        for half in range(2):
            goal, value = regs(turn_key_ref, 128 * half, 16), regs(turn_val_ref, 128 * half, 16)
            goal = [jnp.where((x >> 15) == q, x & 32767, -1) for x in goal]
            for b in range(6, -1, -1):
                route(goal, [value], b, 4, b + 8)
            at = slice(128 * half, 128 * half + 128)
            goal_ref[at, :] = jnp.concatenate(goal, axis=0).T
            move_ref[at, :] = jnp.concatenate(value, axis=0).T
        for u in range(8):
            goal, value = regs(goal_ref, 8 * u, 4, 64), regs(move_ref, 8 * u, 4, 64)
            route(goal, [value], 4, 2, 7)
            route(goal, [value], 3, 2, 6)
            put(goal_ref, 8 * u, goal, 64)
            put(move_ref, 8 * u, value, 64)
        for u in range(4):
            goal, value = regs(goal_ref, 64 * u, 8), regs(move_ref, 64 * u, 8)
            for b in range(5, -1, -1):
                route(goal, [value], b, 3, b)
            write(q, u, [jnp.where(x >= 0, v, 0.0) for x, v in zip(goal, value)])
        return carry

    lax.fori_loop(0, 8, block, 0)


def scatter_kernel(rhs_ref, shift_ref, got_ref, force_ref, inv_ref, to_low_ref, to_up_ref, key_ref, val_ref, rank_ref, turn_key_ref, turn_val_ref):
    unpack_and_merge(got_ref, key_ref, val_ref)
    combine(key_ref, val_ref, rank_ref)
    concentrate(key_ref, val_ref, rank_ref, turn_key_ref, turn_val_ref)

    def write(q, u, values):
        x = 2 * q + u // 2
        for i, value in enumerate(values):
            row, lane = 16 * (u % 2) + 8 * (i // 4), 128 * (i % 4)
            at = (x, slice(row, row + 8), slice(lane, lane + 128))
            force_ref[at] = rhs_ref[at] + value

    distribute(turn_key_ref, turn_val_ref, rank_ref, val_ref, write)

    def finish(x, carry):
        force = force_ref[x]
        inv = 1.0 / (6.0 + shift_ref[x])
        inv_ref[x] = inv
        for which, value in ((0, force), (1, inv)):
            to_low_ref[which, x] = value[0:8]
            to_up_ref[which, x] = value[CY - 8 : CY]
        return carry

    lax.fori_loop(0, CX, finish, 0)


def points_kernel(begin_ref, pos_ref, low_ref, up_ref, nrm_ref, ten_ref, edge_ref, conn_ref, owner_ref, cell_ref, force_ref, send_ref, jump_ref, key_ref, val_ref, goal_ref):
    half = lanes((1, 128)) < 64
    tiles = NPOINT // 128

    def tile(ref, row, t):
        if t < 0:
            return low_ref[row : row + 1, :]
        if t >= tiles:
            return up_ref[row : row + 1, :]
        return ref[row : row + 1, 128 * t : 128 * t + 128]

    for t in range(tiles):
        at = slice(128 * t, 128 * t + 128)
        conn = conn_ref[:, at]
        edge = edge_ref[:, at]
        tension = ten_ref[t : t + 1, :]
        same = (conn >> 7) == begin_ref[0] + t
        spot = conn & 127
        jump = jnp.zeros((1, 128), jnp.float32)
        for c in range(3):
            own = tile(pos_ref, c, t)
            other = jnp.where(half, tile(pos_ref, c, t + 1), tile(pos_ref, c, t - 1))
            shape = conn.shape
            near = jnp.take_along_axis(jnp.broadcast_to(own, shape), spot, axis=1, mode="promise_in_bounds")
            far = jnp.take_along_axis(jnp.broadcast_to(other, shape), spot, axis=1, mode="promise_in_bounds")
            pull = jnp.sum(edge * (jnp.where(same, near, far) - own), axis=0, keepdims=True)
            force = tension * pull
            force_ref[c : c + 1, at] = force
            jump = jump + force * nrm_ref[c : c + 1, at]
        jump_ref[t : t + 1, :] = jump
    pack(owner_ref, cell_ref, jump_ref, begin_ref[1], send_ref, key_ref, val_ref, goal_ref)


def body(pressure_rhs, shift_diag, positions, normals, tension, edge_weight, owner_map, cell_map, connectivity):
    device = lax.axis_index(ALL)
    begin = jnp.stack([device * (NPOINT // 128), device % 2]).astype(jnp.int32)
    ring = [(i, (i + 1) % NDEV) for i in range(NDEV)]
    low = lax.ppermute(positions[:, NPOINT - 128 :], ALL, ring)
    up = lax.ppermute(positions[:, :128], ALL, [(b, a) for a, b in ring])
    flat = (NPOINT // 128, 128)
    whole = pltpu.VMEM(flat, jnp.int32)
    force, send = call(
        points_kernel,
        [(3, NPOINT), (4 * NDEV, 128)],
        (
            begin,
            positions,
            low,
            up,
            normals,
            tension.reshape(flat),
            edge_weight,
            connectivity,
            owner_map.reshape(flat),
            cell_map.reshape(flat),
        ),
        [pltpu.VMEM(flat, jnp.float32), whole, pltpu.VMEM(flat, jnp.float32), whole],
        name="points",
    )
    got = lax.all_to_all(send, ALL, 0, 0, tiled=True)
    block = (CX, CY, CZ)
    list_i, list_f = pltpu.VMEM((256, 128), jnp.int32), pltpu.VMEM((256, 128), jnp.float32)
    forcing, inverse, to_low, to_up = call(
        scatter_kernel,
        [block, block, (2, CX, 8, CZ), (2, CX, 8, CZ)],
        (pressure_rhs, shift_diag, got),
        [list_i, list_f, list_i, list_i, list_f],
        name="scatter",
        limit=8,
    )
    return solve(forcing, inverse, to_low, to_up), force


def solution(mesh):
    point, row = P(ALL), P(None, ALL)
    grid = P("gx", "gy", "gz")
    return jax.shard_map(
        body,
        mesh=mesh,
        in_specs=(grid, grid, row, row, point, row, P(ALL, None), point, row),
        out_specs=(grid, row),
        check_vma=False,
    )
```

```python
import jax
import jax.numpy as jnp
from jax import lax
from jax.experimental import pallas as pl
from jax.experimental.pallas import tpu as pltpu
from jax.sharding import PartitionSpec as P

CX, CY, CZ = 16, 32, 512
W = 3
WC = 5
EX, EY, EZ = CX + 2 * W, CY + 8, CZ + 128
KX, KY = CX // 2 + 2 * WC, 32
T, TE = CZ // 128, EZ // 128
ZB = -(-EX * EY // 128)
ALL = ("gx", "gy", "gz")
NPOINT = 8192
NDEV = 128

CENTRE = 1.125
SPREAD = 0.875
RATIO = CENTRE / SPREAD
SCALE = 1.0 / CENTRE


def factors(sweeps):
    factor, out = 1.0 / RATIO, []
    for _ in range(1, sweeps):
        fresh = 1.0 / (2.0 * RATIO - factor)
        out.append((fresh * factor, 2.0 * fresh / SPREAD))
        factor = fresh
    return out


def call(kernel, outs, operands, scratch=(), name=None, limit=4, alias=None, far=(), far_out=()):
    vmem, anywhere = pl.BlockSpec(memory_space=pltpu.VMEM), pl.BlockSpec(memory_space=pltpu.HBM)
    specs = [
        pl.BlockSpec(memory_space=pltpu.SMEM)
        if o.dtype == jnp.int32 and o.ndim == 1
        else (anywhere if i in far else vmem)
        for i, o in enumerate(operands)
    ]
    return pl.pallas_call(
        kernel,
        out_shape=[jax.ShapeDtypeStruct(s, jnp.float32) for s in outs],
        in_specs=specs,
        out_specs=[anywhere if i in far_out else vmem for i in range(len(outs))],
        scratch_shapes=list(scratch),
        compiler_params=pltpu.CompilerParams(vmem_limit_bytes=limit << 20),
        input_output_aliases=alias or {},
        name=name,
    )(*operands)


def lanes(shape):
    return lax.broadcasted_iota(jnp.int32, shape, len(shape) - 1)


def rows(shape):
    return lax.broadcasted_iota(jnp.int32, shape, len(shape) - 2)


def span(x, n):
    return pl.ds(pl.multiple_of(n * x, 8), n)


def get(ref, x, n):
    return jnp.concatenate([ref[t, span(x, n), :] for t in range(TE)], axis=1)


def put_plane(ref, x, value):
    n = value.shape[0]
    for t in range(TE):
        ref[t, span(x, n), :] = value[:, 128 * t : 128 * t + 128]


def neighbours(ref, x, n, step):
    plane = get(ref, x, n)
    nz = plane.shape[1]
    beside = get(ref, x - 1, n) + get(ref, x + 1, n)
    beside = beside + (pltpu.roll(plane, 1, 0) + pltpu.roll(plane, n - 1, 0))
    return plane, beside + (pltpu.roll(plane, step, 1) + pltpu.roll(plane, nz - step, 1))


def planes(first, last, body, group=2):
    count = (last - first) // group

    def step(i, carry):
        for j in range(group):
            body(first + group * i + j)
        return carry

    lax.fori_loop(0, count, step, 0)
    for x in range(first + group * count, last):
        body(x)


def x_faces(force_ref, inv_ref, up_ref, low_ref, to_low_ref, to_up_ref):
    for which, ref in ((0, force_ref), (1, inv_ref)):
        for out, first in ((to_low_ref, 0), (to_up_ref, CX - W)):
            for t in range(T):
                for p in range(W):
                    x = first + p
                    out[which, t, EY * p : EY * p + CY, :] = ref[t, CY * x : CY * x + CY, :]
                    out[which, t, EY * p + CY : EY * p + EY, :] = jnp.zeros((8, 128), jnp.float32)
                    for r in range(W):
                        at = EY * p + CY + r
                        out[which, t, at : at + 1, :] = up_ref[which, r, t, x : x + 1, :]
                        at = EY * p + EY - W + r
                        out[which, t, at : at + 1, :] = low_ref[which, r, t, x : x + 1, :]


def assemble(force_ref, inv_ref, yup_ref, ylow_ref, xup_ref, xlow_ref, f_ref, v_ref, to_low_ref, to_up_ref):
    for which, (src, dst) in enumerate(((force_ref, f_ref), (inv_ref, v_ref))):
        for t in range(T):
            dst[t, 0 : EY * W, :] = xlow_ref[which, t]
            dst[t, EY * (W + CX) :, :] = xup_ref[which, t]
            for x in range(CX):
                at = EY * (W + x)
                dst[t, at : at + CY, :] = src[t, CY * x : CY * x + CY, :]
            at = EY * W + CY
            for r in range(W):
                dst[t, pl.ds(at + r, CX, EY), :] = yup_ref[which, r, t]
                dst[t, pl.ds(at + 8 - W + r, CX, EY), :] = ylow_ref[which, r, t]
            for r in range(W, 8 - W):
                dst[t, pl.ds(at + r, CX, EY), :] = jnp.zeros((CX, 128), jnp.float32)
    spot = lanes((128, 128))
    for j in range(ZB):
        first = min(128 * j, EX * EY - 128)
        at = slice(first, first + 128)
        mixed = jnp.where(
            spot < 16,
            f_ref[0, at, :],
            jnp.where(
                spot < 32,
                pltpu.roll(v_ref[0, at, :], 16, 1),
                jnp.where(spot < 48, pltpu.roll(f_ref[T - 1, at, :], 48, 1), pltpu.roll(v_ref[T - 1, at, :], 64, 1)),
            ),
        )
        turned = mixed.T
        to_low_ref[:, 128 * j : 128 * j + 128] = turned[0:32]
        to_up_ref[:, 128 * j : 128 * j + 128] = turned[32:64]


def smooth_kernel(_fin_ref, _vin_ref, zup_ref, zlow_ref, f_ref, v_ref, a_ref, to_low_ref, to_up_ref, coarse_ref, b_ref, tmp_ref):
    gap = jnp.zeros((96, 128), jnp.float32)
    for j in range(ZB):
        first = min(128 * j, EX * EY - 128)
        at = slice(128 * j, 128 * j + 128)
        for dst, part in ((f_ref, slice(0, 16)), (v_ref, slice(16, 32))):
            stack = jnp.concatenate([zup_ref[part, at], gap, zlow_ref[part, at]], axis=0)
            dst[T, first : first + 128, :] = stack.T

    def start(x):
        put_plane(a_ref, x, get(v_ref, x, EY) * get(f_ref, x, EY) * SCALE)

    planes(0, EX, start)
    (a1, b1), (a2, b2) = factors(3)

    def second(x):
        plane, beside = neighbours(a_ref, x, EY, 1)
        left = get(v_ref, x, EY) * (get(f_ref, x, EY) + beside) - plane
        put_plane(b_ref, x, (1.0 + a1) * plane + b1 * left)

    planes(1, EX - 1, second)

    def third(x):
        plane, beside = neighbours(b_ref, x, EY, 1)
        left = get(v_ref, x, EY) * (get(f_ref, x, EY) + beside) - plane
        put_plane(a_ref, x, plane + a2 * (plane - get(a_ref, x, EY)) + b2 * left)

    planes(2, EX - 2, third)
    even = lanes((CY // 2, EZ)) % 2 == 0

    def restrict(xc):
        total, weight = [], []
        for half in range(2):
            x = W + 2 * xc + half
            plane, beside = neighbours(a_ref, x, EY, 1)
            inv = get(v_ref, x, EY)[0:CY]
            diag = jnp.where(inv > 0.0, 1.0 / inv, 0.0)
            total.append((get(f_ref, x, EY) + beside)[0:CY] - diag * plane[0:CY])
            weight.append(diag)

        def pairs(value, slot):
            value = value + pltpu.roll(value, EZ - 1, 1)
            parts = []
            for t in range(TE):
                tmp_ref[slot, t] = value[:, 128 * t : 128 * t + 128]
                parts.append(tmp_ref[slot, t, pl.ds(0, CY // 2, 2)] + tmp_ref[slot, t, pl.ds(1, CY // 2, 2)])
            return jnp.concatenate(parts, axis=1)

        rhs = 0.5 * pairs(total[0] + total[1], 0)
        whole = pairs(weight[0] + weight[1], 1)
        inv = jnp.where(whole > 0.0, 1.0 / (6.0 + 0.5 * (whole - 48.0)), 0.0)
        put_plane(coarse_ref, xc, jnp.where(even, rhs, pltpu.roll(inv, 1, 1)))

    planes(0, CX // 2, restrict, 1)
    for t in range(TE):
        for r in range(WC):
            at = 8 * (r * TE + t)
            to_low_ref[at : at + 8, :] = coarse_ref[t, pl.ds(r, CX // 2, CY // 2), :]
            to_up_ref[at : at + 8, :] = coarse_ref[t, pl.ds(CY // 2 - WC + r, CX // 2, CY // 2), :]
        for r in range(W):
            at = 8 * WC * TE + 16 * (r * TE + t)
            to_low_ref[at : at + 16, :] = a_ref[t, pl.ds(EY * W + r, CX, EY), :]
            to_up_ref[at : at + 16, :] = a_ref[t, pl.ds(EY * W + CY - W + r, CX, EY), :]


def coarse_faces(own_ref, a_ref, up_ref, low_ref, to_low_ref, to_up_ref):
    none = jnp.zeros((8, 128), jnp.float32)
    for t in range(TE):
        for out, first in ((to_low_ref, 0), (to_up_ref, CX // 2 - WC)):
            for p in range(WC):
                x = first + p
                out[t, KY * p : KY * p + 16, :] = own_ref[t, 16 * x : 16 * x + 16, :]
                out[t, KY * p + 16 : KY * p + 24, :] = none
                out[t, KY * p + 24 : KY * p + 32, :] = none
            for r in range(WC):
                at = 8 * (r * TE + t) + first
                out[t, pl.ds(16 + r, WC, KY), :] = up_ref[at : at + WC, :]
                out[t, pl.ds(KY - WC + r, WC, KY), :] = low_ref[at : at + WC, :]
        base = KY * WC
        for out, first in ((to_low_ref, 0), (to_up_ref, CX - W)):
            for p in range(W):
                at, x = base + EY * p, EY * (W + first + p)
                out[t, at : at + CY, :] = a_ref[t, x : x + CY, :]
                out[t, at + CY : at + EY, :] = none
            for r in range(W):
                at = 8 * WC * TE + 16 * (r * TE + t) + first
                out[t, pl.ds(base + CY + r, W, EY), :] = up_ref[at : at + W, :]
                out[t, pl.ds(base + EY - W + r, W, EY), :] = low_ref[at : at + W, :]


def final_kernel(f_ref, v_ref, ain_ref, own_ref, yup_ref, ylow_ref, xup_ref, xlow_ref, out_ref, a_ref, b_ref, cb_ref, cv_ref, ca_ref, cc_ref, tmp_ref, res_ref, sems):
    half = CX // 2
    base = KY * WC
    for t in range(TE):
        cc_ref[t, 0:base, :] = xlow_ref[t, 0:base, :]
        cc_ref[t, KY * (WC + half) :, :] = xup_ref[t, 0:base, :]
        a_ref[t, 0 : EY * W, :] = xlow_ref[t, base:, :]
        a_ref[t, EY * (W + CX) :, :] = xup_ref[t, base:, :]
        for x in range(half):
            at = KY * (WC + x)
            cc_ref[t, at : at + 16, :] = own_ref[t, 16 * x : 16 * x + 16, :]
        at = KY * WC + 16
        for r in range(WC):
            src = slice(8 * (r * TE + t), 8 * (r * TE + t) + 8)
            cc_ref[t, pl.ds(at + r, half, KY), :] = yup_ref[src, :]
            cc_ref[t, pl.ds(at + 16 - WC + r, half, KY), :] = ylow_ref[src, :]
        for r in range(WC, 16 - WC):
            cc_ref[t, pl.ds(at + r, half, KY), :] = jnp.zeros((half, 128), jnp.float32)
        at = EY * W + CY
        for r in range(W):
            first = 8 * WC * TE + 16 * (r * TE + t)
            a_ref[t, pl.ds(at + r, CX, EY), :] = yup_ref[first : first + 16, :]
            a_ref[t, pl.ds(at + 8 - W + r, CX, EY), :] = ylow_ref[first : first + 16, :]
        for r in range(W, 8 - W):
            a_ref[t, pl.ds(at + r, CX, EY), :] = jnp.zeros((CX, 128), jnp.float32)
    even = lanes((KY, EZ)) % 2 == 0
    (a1, b1), (a2, b2), (a3, b3) = factors(4)

    def start(x):
        both = get(cc_ref, x, KY)
        right = jnp.where(even, both, pltpu.roll(both, 1, 1))
        inv = jnp.where(even, pltpu.roll(both, EZ - 1, 1), both)
        put_plane(cb_ref, x, right)
        put_plane(cv_ref, x, inv)
        put_plane(ca_ref, x, inv * right * SCALE)

    planes(0, KX, start)

    def sweep(src, dst, first, last, a, b, fresh):
        def body(x):
            plane, beside = neighbours(src, x, KY, 2)
            left = get(cv_ref, x, KY) * (get(cb_ref, x, KY) + beside) - plane
            step = plane if fresh else plane - get(dst, x, KY)
            put_plane(dst, x, plane + a * step + b * left)

        planes(first, last, body)

    sweep(ca_ref, cc_ref, 1, KX - 1, a1, b1, True)
    sweep(cc_ref, ca_ref, 2, KX - 2, a2, b2, False)
    sweep(ca_ref, cc_ref, 3, KX - 3, a3, b3, False)
    low = rows((8, 128)) < 4

    def spread(x, src):
        xc = (x - W + 2 * WC) // 2
        for t in range(TE):
            coarse = cc_ref[t, span(xc, KY), :]
            tmp_ref[t, pl.ds(0, 32, 2)] = coarse
            tmp_ref[t, pl.ds(1, 32, 2)] = coarse
            at = EY * x
            own, rim = pl.ds(pl.multiple_of(at, 8), CY), pl.ds(pl.multiple_of(at + CY, 8), 8)
            a_ref[t, own, :] = src[t, own, :] + tmp_ref[t, 0:CY]
            a_ref[t, rim, :] = a_ref[t, rim, :] + jnp.where(low, tmp_ref[t, 32:40], tmp_ref[t, 56:64])

    planes(0, W, lambda x: spread(x, a_ref), 1)
    planes(W, W + CX, lambda x: spread(x, ain_ref), 1)
    planes(W + CX, EX, lambda x: spread(x, a_ref), 1)
    (a1, b1), (a2, b2) = factors(3)

    def first(x):
        plane, beside = neighbours(a_ref, x, EY, 1)
        left = get(v_ref, x, EY) * (get(f_ref, x, EY) + beside) - plane
        put_plane(b_ref, x, plane + SCALE * left)

    planes(1, EX - 1, first)

    def second(x):
        plane, beside = neighbours(b_ref, x, EY, 1)
        left = get(v_ref, x, EY) * (get(f_ref, x, EY) + beside) - plane
        put_plane(a_ref, x, plane + a1 * (plane - get(a_ref, x, EY)) + b1 * left)

    planes(2, EX - 2, second)

    def third(x):
        plane, beside = neighbours(a_ref, x, EY, 1)
        left = get(v_ref, x, EY) * (get(f_ref, x, EY) + beside) - plane
        full = plane + a2 * (plane - get(b_ref, x, EY)) + b2 * left
        res_ref[x - W] = full[0:CY, 0:CZ]

    copies = []
    for i in range(4):
        at = pl.ds(4 * i, 4)
        planes(W + 4 * i, W + 4 * i + 4, third)
        copies.append(pltpu.make_async_copy(res_ref.at[at], out_ref.at[at], sems.at[i]))
        copies[-1].start()
    for copy in copies:
        copy.wait()


def swap(low, high, axis):
    count = lax.axis_size(axis)
    up = [(i, i + 1) for i in range(count - 1)]
    return lax.ppermute(low, axis, [(b, a) for a, b in up]), lax.ppermute(high, axis, up)


def solve(forcing, inverse, to_low, to_up):
    yup, ylow = swap(to_low, to_up, "gy")
    face = (2, T, W * EY, 128)
    xs = call(x_faces, [face, face], (forcing, inverse, yup, ylow), name="x_faces")
    xup, xlow = swap(*xs, "gx")
    ext = (TE, EX * EY, 128)
    f, v, zl, zu = call(
        assemble,
        [ext, ext, (32, 128 * ZB), (32, 128 * ZB)],
        (forcing, inverse, yup, ylow, xup, xlow),
        name="assemble",
    )
    zup, zlow = swap(zl, zu, "gz")
    cy, cx = (8 * TE * (WC + 2 * W), 128), (TE, KY * WC + EY * W, 128)
    f, v, a, yl, yu, own = call(
        smooth_kernel,
        [ext, ext, ext, cy, cy, (TE, CX // 2 * CY // 2, 128)],
        (f, v, zup, zlow),
        [pltpu.VMEM(ext, jnp.float32), pltpu.VMEM((2, TE, CY, 128), jnp.float32)],
        name="smooth",
        limit=8,
        alias={0: 0, 1: 1},
    )
    yup, ylow = swap(yl, yu, "gy")
    xs = call(coarse_faces, [cx, cx], (own, a, yup, ylow), name="coarse_faces")
    xup, xlow = swap(*xs, "gx")
    cext = pltpu.VMEM((TE, KX * KY, 128), jnp.float32)
    return call(
        final_kernel,
        [(CX, CY, CZ)],
        (f, v, a, own, yup, ylow, xup, xlow),
        [pltpu.VMEM(ext, jnp.float32)] * 2
        + [cext] * 4
        + [pltpu.VMEM((TE, 64, 128), jnp.float32), pltpu.VMEM((CX, CY, CZ), jnp.float32), pltpu.SemaphoreType.DMA((4,))],
        name="final",
        limit=20,
        far_out=(0,),
    )[0]


def bit_of(b, nv):
    if b < 3:
        return (lax.broadcasted_iota(jnp.int32, (8, 128), 0) >> b) & 1
    return (lax.broadcasted_iota(jnp.int32, (8, 128), 1) >> (b - 3 - nv)) & 1


def in_list(b, nv):
    return 3 <= b < 3 + nv


def across(x, b, nv, high):
    axis, size, d = (0, 8, 1 << b) if b < 3 else (1, 128, 1 << (b - 3 - nv))
    if 2 * d == size:
        return pltpu.roll(x, d, axis)
    return jnp.where(high, pltpu.roll(x, d, axis), pltpu.roll(x, size - d, axis))


def exchange(keys, values, b, nv):
    if in_list(b, nv):
        d = 1 << (b - 3)
        for u in range(len(keys)):
            if u & d:
                continue
            low, high = keys[u], keys[u + d]
            turn = low > high
            keys[u], keys[u + d] = jnp.minimum(low, high), jnp.maximum(low, high)
            a, c = values[u], values[u + d]
            values[u], values[u + d] = jnp.where(turn, c, a), jnp.where(turn, a, c)
        return
    high = bit_of(b, nv) != 0
    others = [across(key, b, nv, high) for key in keys]
    loads = [across(value, b, nv, high) for value in values]
    for u, other in enumerate(others):
        key = keys[u]
        keys[u] = jnp.where(high, jnp.maximum(key, other), jnp.minimum(key, other))
        values[u] = jnp.where(keys[u] != key, loads[u], values[u])


SIGN = -(1 << 31)


def route(goal, loads, b, nv, g):
    mask, one = jnp.int32(SIGN | (1 << g)), 1 << g
    if in_list(b, nv):
        d = 1 << (b - 3)
        for u in range(len(goal)):
            if u & d:
                continue
            low, high = goal[u], goal[u + d]
            ml, mh = low & mask, high & mask
            stay_l, stay_h = ml == 0, mh == one
            goal[u] = jnp.where(stay_l, low, jnp.where(mh == 0, high, -1))
            goal[u + d] = jnp.where(stay_h, high, jnp.where(ml == one, low, -1))
            for load in loads:
                a, c = load[u], load[u + d]
                load[u], load[u + d] = jnp.where(stay_l, a, c), jnp.where(stay_h, c, a)
        return
    place = bit_of(b, nv)
    high = place != 0
    place = place << g
    others = [across(x, b, nv, high) for x in goal]
    moved = [[across(x, b, nv, high) for x in load] for load in loads]
    for u, other in enumerate(others):
        own = goal[u]
        stay = (own & mask) == place
        goal[u] = jnp.where(stay, own, jnp.where((other & mask) == place, other, -1))
        for load, move in zip(loads, moved):
            load[u] = jnp.where(stay, load[u], move[u])


NONE = 1 << 18


def pack(owner_ref, cell_ref, jump_ref, turn, out_ref, key_ref, val_ref, goal_ref):
    nv = 3
    keys, values = [], []
    for u in range(8):
        at = slice(8 * u, 8 * u + 8)
        cell = cell_ref[at, :]
        mixed = (
            ((cell >> 15) << 15)
            | ((cell & 127) << 8)
            | ((cell >> 14) & 1) << 7
            | ((cell >> 12) & 3) << 5
            | ((cell >> 7) & 3) << 3
            | (cell >> 9) & 7
        )
        mixed = mixed ^ (turn * (NONE - 1))
        keys.append((owner_ref[at, :] << 18) | mixed)
        values.append(jump_ref[at, :])
    for k in range(1, 14):

        def flip(keys):
            if k == 13:
                return keys
            if in_list(k, nv):
                return [~key if (u >> (k - 3)) & 1 else key for u, key in enumerate(keys)]
            turned = -bit_of(k, nv)
            return [key ^ turned for key in keys]

        keys = flip(keys)
        for b in range(k - 1, -1, -1):
            exchange(keys, values, b, nv)
        keys = flip(keys)
    owners = [key >> 18 for key in keys]
    spot = 64 * lanes((8, 128)) + rows((8, 128))
    tail = [(owner << 13) | (8 * u + spot) for u, owner in enumerate(owners)]
    runs = list(tail)
    for b in range(13):
        if in_list(b, nv):
            d = 1 << (b - 3)
            other = [tail[u ^ d] for u in range(8)]
        else:
            d, high = 0, bit_of(b, nv) != 0
            other = [across(x, b, nv, high) for x in tail]
        for u in range(8):
            same = (other[u] ^ tail[u]) < 8192
            joins = (other[u] ^ runs[u]) < 8192
            if not d:
                runs[u] = jnp.where(high & joins, other[u], runs[u])
                tail[u] = jnp.where(high == same, other[u], tail[u])
            elif u & d:
                runs[u] = jnp.where(joins, other[u], runs[u])
                tail[u] = jnp.where(same, other[u], tail[u])
            else:
                tail[u] = jnp.where(same, tail[u], other[u])
    for u in range(8):
        at = slice(8 * u, 8 * u + 8)
        goal_ref[at, :] = 256 * owners[u] + 8 * u + spot - (runs[u] & 8191)
        key_ref[at, :] = (keys[u] & (NONE - 1)) ^ (turn * (NONE - 1))
        val_ref[at, :] = values[u]
    empty = NONE * (1 - turn) - turn

    def block(q, carry):
        sets = []
        for i in range(2):
            goal, key, value = [], [], []
            for u in range(8):
                at = slice(8 * u, 8 * u + 8)
                g = goal_ref[at, :]
                goal.append(jnp.where((g >> 13) == 2 * q + i, g & 8191, -1))
                key.append(key_ref[at, :])
                value.append(val_ref[at, :])
            sets.append((goal, key, value))
        for b in range(12, -1, -1):
            for goal, key, value in sets:
                route(goal, [key, value], b, nv, b)
        for i, (goal, key, value) in enumerate(sets):
            full = [g >= 0 for g in goal]
            parts = [jnp.where(f, v, 0.0) for f, v in zip(full, value)]
            parts += [jnp.where(f, c, empty).astype(jnp.float32) for f, c in zip(full, key)]
            first = pl.multiple_of(256 * q + 128 * i, 128)
            out_ref[pl.ds(first, 128), :] = jnp.concatenate(parts, axis=0).T
        return carry

    lax.fori_loop(0, 2, block, 0)


def regs(ref, first, count, step=8):
    return [ref[pl.ds(first + step * u, 8), :] for u in range(count)]


def put(ref, first, parts, step=8):
    for u, part in enumerate(parts):
        ref[pl.ds(first + step * u, 8), :] = part


def shifted(x, d):
    if d >= 256:
        return pltpu.roll(x, d // 256, 1)
    y = pltpu.roll(x, d, 0)
    head = max(d, 8)
    edge = jnp.where(rows((head, 128)) < d, pltpu.roll(y[:head], 1, 1), y[:head])
    return jnp.concatenate([edge, y[head:]], axis=0) if head < 256 else edge


def unpack_and_merge(got_ref, key_ref, val_ref):
    nv = 5
    for quarter in range(4):
        turned = got_ref[pl.ds(quarter, 128, 4), :].T
        val_ref[64 * quarter : 64 * quarter + 64, :] = turned[:64]
        key_ref[64 * quarter : 64 * quarter + 64, :] = turned[64:].astype(jnp.int32)
    before = 0
    for k in range(9, 16):
        turned = -bit_of(k, nv) if k < 15 else 0
        change = turned ^ before
        before = turned
        for b in range(k - 1, 7, -1):
            for half in range(2):
                keys, values = regs(key_ref, 128 * half, 16), regs(val_ref, 128 * half, 16)
                if b == k - 1:
                    keys = [key ^ change for key in keys]
                exchange(keys, values, b, nv)
                put(key_ref, 128 * half, keys)
                put(val_ref, 128 * half, values)
        for u in range(8):
            keys, values = regs(key_ref, 8 * u, 4, 64), regs(val_ref, 8 * u, 4, 64)
            for b in (4, 3):
                exchange(keys, values, b, 2)
            put(key_ref, 8 * u, keys, 64)
            put(val_ref, 8 * u, values, 64)
        for u in range(4):
            keys, values = regs(key_ref, 64 * u, 8), regs(val_ref, 64 * u, 8)
            for b in range(5, -1, -1):
                exchange(keys, values, b, 3)
            put(key_ref, 64 * u, keys)
            put(val_ref, 64 * u, values)


def combine(key_ref, val_ref, rank_ref):
    spot = rows((256, 128)) + 256 * lanes((256, 128))

    def gather(d):
        key, value = key_ref[...], val_ref[...]
        same = (shifted(key, d) == key) & (spot >= d)
        val_ref[...] = value + jnp.where(same, shifted(value, d), 0.0)

    for d in (1, 2, 4):
        gather(d)
    key = key_ref[...]
    real = (key >= 0) & (key < NONE)
    long = jnp.where(real & (shifted(key, 8) == key) & (spot >= 8), 1.0, 0.0)

    @pl.when(jnp.max(long) > 0.0)
    def _():
        for e in range(3, 15):
            gather(1 << e)

    after = pltpu.roll(key, 255, 0)
    edge = jnp.where(rows((8, 128)) == 7, pltpu.roll(after[248:], 127, 1), after[248:])
    after = jnp.concatenate([after[:248], edge], axis=0)
    last = real & ((after != key) | (spot == 32767))
    one = lambda test: jnp.where(test, 1.0, 0.0).astype(jnp.bfloat16)
    mask = one(last)
    dot = lambda a, b: jnp.dot(a, b, preferred_element_type=jnp.float32)
    within = dot(one(rows((256, 256)) > lanes((256, 256))), mask)
    totals = dot(jnp.ones((256, 256), jnp.bfloat16), mask).astype(jnp.bfloat16)
    before = dot(totals, one(rows((128, 128)) < lanes((128, 128))))
    rank_ref[...] = jnp.where(last, (within + before).astype(jnp.int32), -1)


def concentrate(key_ref, val_ref, rank_ref, turn_key_ref, turn_val_ref):
    refs = (rank_ref, key_ref, val_ref)

    def stages(first, count, step, bits):
        goal, key, value = (regs(r, first, count, step) for r in refs)
        for b, nv, g in bits:
            route(goal, [key, value], b, nv, g)
        for r, parts in zip(refs, (goal, key, value)):
            put(r, first, parts, step)

    for u in range(4):
        stages(64 * u, 8, 8, [(b, 3, b) for b in range(6)])
    for u in range(8):
        stages(8 * u, 4, 64, [(3, 2, 6), (4, 2, 7)])
    for b in range(8, 15):
        for half in range(2):
            stages(128 * half, 16, 8, [(b, 5, b)])
    for half in range(2):
        at = slice(128 * half, 128 * half + 128)
        turn_key_ref[at, :] = jnp.where(rank_ref[at, :] >= 0, key_ref[at, :], -1).T
        turn_val_ref[at, :] = val_ref[at, :].T


def distribute(turn_key_ref, turn_val_ref, goal_ref, move_ref, write):
    def block(q, carry):
        for half in range(2):
            goal, value = regs(turn_key_ref, 128 * half, 16), regs(turn_val_ref, 128 * half, 16)
            goal = [jnp.where((x >> 15) == q, x & 32767, -1) for x in goal]
            for b in range(6, -1, -1):
                route(goal, [value], b, 4, b + 8)
            at = slice(128 * half, 128 * half + 128)
            goal_ref[at, :] = jnp.concatenate(goal, axis=0).T
            move_ref[at, :] = jnp.concatenate(value, axis=0).T
        for u in range(8):
            goal, value = regs(goal_ref, 8 * u, 4, 64), regs(move_ref, 8 * u, 4, 64)
            route(goal, [value], 4, 2, 7)
            route(goal, [value], 3, 2, 6)
            put(goal_ref, 8 * u, goal, 64)
            put(move_ref, 8 * u, value, 64)
        for u in range(4):
            goal, value = regs(goal_ref, 64 * u, 8), regs(move_ref, 64 * u, 8)
            for b in range(5, -1, -1):
                route(goal, [value], b, 3, b)
            write(q, u, [jnp.where(x >= 0, v, 0.0) for x, v in zip(goal, value)])
        return carry

    lax.fori_loop(0, 8, block, 0)


def scatter_kernel(rhs_hbm, shift_hbm, got_ref, force_ref, inv_ref, to_low_ref, to_up_ref, rhs_ref, shift_ref, key_ref, val_ref, rank_ref, turn_key_ref, turn_val_ref, sems):
    rhs_copy = pltpu.make_async_copy(rhs_hbm, rhs_ref, sems.at[0])
    shift_copy = pltpu.make_async_copy(shift_hbm, shift_ref, sems.at[1])
    rhs_copy.start()
    shift_copy.start()
    unpack_and_merge(got_ref, key_ref, val_ref)
    combine(key_ref, val_ref, rank_ref)
    concentrate(key_ref, val_ref, rank_ref, turn_key_ref, turn_val_ref)
    rhs_copy.wait()
    shift_copy.wait()

    def write(q, u, values):
        x = 2 * q + u // 2
        for i, value in enumerate(values):
            row, t = 16 * (u % 2) + 8 * (i // 4), i % 4
            at = (x, slice(row, row + 8), slice(128 * t, 128 * t + 128))
            to = (t, pl.ds(pl.multiple_of(CY * x + row, 8), 8))
            force_ref[to] = rhs_ref[at] + value
            inv_ref[to] = 1.0 / (6.0 + shift_ref[at])

    distribute(turn_key_ref, turn_val_ref, rank_ref, val_ref, write)
    for which, ref in ((0, force_ref), (1, inv_ref)):
        for r in range(W):
            for t in range(T):
                to_low_ref[which, r, t] = ref[t, pl.ds(r, CX, CY), :]
                to_up_ref[which, r, t] = ref[t, pl.ds(CY - W + r, CX, CY), :]


def points_kernel(begin_ref, low_ref, up_ref, pos_hbm, nrm_hbm, ten_hbm, edge_hbm, conn_hbm, owner_hbm, cell_hbm, force_ref, send_ref, pos_ref, nrm_ref, ten_ref, edge_ref, conn_ref, owner_ref, cell_ref, jump_ref, key_ref, val_ref, goal_ref, sems):
    far = (pos_hbm, nrm_hbm, ten_hbm, edge_hbm, conn_hbm, owner_hbm, cell_hbm)
    near = (pos_ref, nrm_ref, ten_ref, edge_ref, conn_ref, owner_ref, cell_ref)
    copies = [pltpu.make_async_copy(a, b, sems.at[i]) for i, (a, b) in enumerate(zip(far, near))]
    for copy in copies:
        copy.start()
    for copy in copies:
        copy.wait()
    half = lanes((1, 128)) < 64
    tiles = NPOINT // 128

    def tile(ref, row, t):
        if t < 0:
            return low_ref[row : row + 1, :]
        if t >= tiles:
            return up_ref[row : row + 1, :]
        return ref[row : row + 1, 128 * t : 128 * t + 128]

    for t in range(tiles):
        at = slice(128 * t, 128 * t + 128)
        conn = conn_ref[:, at]
        edge = edge_ref[:, at]
        tension = ten_ref[t : t + 1, :]
        same = (conn >> 7) == begin_ref[0] + t
        spot = conn & 127
        jump = jnp.zeros((1, 128), jnp.float32)
        for c in range(3):
            own = tile(pos_ref, c, t)
            other = jnp.where(half, tile(pos_ref, c, t + 1), tile(pos_ref, c, t - 1))
            shape = conn.shape
            near = jnp.take_along_axis(jnp.broadcast_to(own, shape), spot, axis=1, mode="promise_in_bounds")
            far = jnp.take_along_axis(jnp.broadcast_to(other, shape), spot, axis=1, mode="promise_in_bounds")
            pull = jnp.sum(edge * (jnp.where(same, near, far) - own), axis=0, keepdims=True)
            force = tension * pull
            force_ref[c : c + 1, at] = force
            jump = jump + force * nrm_ref[c : c + 1, at]
        jump_ref[t : t + 1, :] = jump
    pack(owner_ref, cell_ref, jump_ref, begin_ref[1], send_ref, key_ref, val_ref, goal_ref)


def body(pressure_rhs, shift_diag, positions, normals, tension, edge_weight, owner_map, cell_map, connectivity):
    device = lax.axis_index(ALL)
    begin = jnp.stack([device * (NPOINT // 128), device % 2]).astype(jnp.int32)
    ring = [(i, (i + 1) % NDEV) for i in range(NDEV)]
    low = lax.ppermute(positions[:, NPOINT - 128 :], ALL, ring)
    up = lax.ppermute(positions[:, :128], ALL, [(b, a) for a, b in ring])
    flat = (NPOINT // 128, 128)
    whole = pltpu.VMEM(flat, jnp.int32)
    force, send = call(
        points_kernel,
        [(3, NPOINT), (4 * NDEV, 128)],
        (
            begin,
            low,
            up,
            positions,
            normals,
            tension.reshape(flat),
            edge_weight,
            connectivity,
            owner_map.reshape(flat),
            cell_map.reshape(flat),
        ),
        [pltpu.VMEM((3, NPOINT), jnp.float32)] * 2
        + [pltpu.VMEM(flat, jnp.float32), pltpu.VMEM((6, NPOINT), jnp.float32), pltpu.VMEM((6, NPOINT), jnp.int32)]
        + [whole, whole, pltpu.VMEM(flat, jnp.float32), whole, pltpu.VMEM(flat, jnp.float32), whole]
        + [pltpu.SemaphoreType.DMA((7,))],
        far=range(3, 10),
        name="points",
    )
    got = lax.all_to_all(send, ALL, 0, 0, tiled=True)
    block = pltpu.VMEM((CX, CY, CZ), jnp.float32)
    list_i, list_f = pltpu.VMEM((256, 128), jnp.int32), pltpu.VMEM((256, 128), jnp.float32)
    own, face = (T, CX * CY, 128), (2, W, T, CX, 128)
    forcing, inverse, to_low, to_up = call(
        scatter_kernel,
        [own, own, face, face],
        (pressure_rhs, shift_diag, got),
        [block, block, list_i, list_f, list_i, list_i, list_f, pltpu.SemaphoreType.DMA((2,))],
        name="scatter",
        limit=8,
        far=(0, 1),
    )
    return solve(forcing, inverse, to_low, to_up), force


def solution(mesh):
    point, row = P(ALL), P(None, ALL)
    grid = P("gx", "gy", "gz")
    return jax.shard_map(
        body,
        mesh=mesh,
        in_specs=(grid, grid, row, row, point, row, P(ALL, None), point, row),
        out_specs=(grid, row),
        check_vma=False,
    )
```

```python
import jax
import jax.numpy as jnp
from jax import lax
from jax.experimental import pallas as pl
from jax.experimental.pallas import tpu as pltpu
from jax.sharding import PartitionSpec as P

CX, CY, CZ = 16, 32, 512
W = 3
WC = 5
EX, EY, EZ = CX + 2 * W, CY + 8, CZ + 128
KX, KY = CX // 2 + 2 * WC, 32
T, TE = CZ // 128, EZ // 128
ZB = -(-EX * EY // 128)
ALL = ("gx", "gy", "gz")
NPOINT = 8192
NDEV = 128

CENTRE = 1.125
SPREAD = 0.875
RATIO = CENTRE / SPREAD
SCALE = 1.0 / CENTRE


def factors(sweeps):
    factor, out = 1.0 / RATIO, []
    for _ in range(1, sweeps):
        fresh = 1.0 / (2.0 * RATIO - factor)
        out.append((fresh * factor, 2.0 * fresh / SPREAD))
        factor = fresh
    return out


def call(kernel, outs, operands, scratch=(), name=None, limit=4, alias=None, far=(), far_out=()):
    vmem, anywhere = pl.BlockSpec(memory_space=pltpu.VMEM), pl.BlockSpec(memory_space=pltpu.HBM)
    specs = [
        pl.BlockSpec(memory_space=pltpu.SMEM)
        if o.dtype == jnp.int32 and o.ndim == 1
        else (anywhere if i in far else vmem)
        for i, o in enumerate(operands)
    ]
    return pl.pallas_call(
        kernel,
        out_shape=[jax.ShapeDtypeStruct(s, jnp.float32) for s in outs],
        in_specs=specs,
        out_specs=[anywhere if i in far_out else vmem for i in range(len(outs))],
        scratch_shapes=list(scratch),
        compiler_params=pltpu.CompilerParams(vmem_limit_bytes=limit << 20),
        input_output_aliases=alias or {},
        name=name,
    )(*[pltpu.with_memory_space_constraint(o, pltpu.HBM) if i in far else o for i, o in enumerate(operands)])


def lanes(shape):
    return lax.broadcasted_iota(jnp.int32, shape, len(shape) - 1)


def rows(shape):
    return lax.broadcasted_iota(jnp.int32, shape, len(shape) - 2)


def span(x, n):
    return pl.ds(pl.multiple_of(n * x, 8), n)


def get(ref, x, n):
    return jnp.concatenate([ref[t, span(x, n), :] for t in range(TE)], axis=1)


def put_plane(ref, x, value):
    n = value.shape[0]
    for t in range(TE):
        ref[t, span(x, n), :] = value[:, 128 * t : 128 * t + 128]


def neighbours(ref, x, n, step):
    plane = get(ref, x, n)
    nz = plane.shape[1]
    beside = get(ref, x - 1, n) + get(ref, x + 1, n)
    beside = beside + (pltpu.roll(plane, 1, 0) + pltpu.roll(plane, n - 1, 0))
    return plane, beside + (pltpu.roll(plane, step, 1) + pltpu.roll(plane, nz - step, 1))


GROUP = 4


def planes(first, last, body, group=0):
    group = group or GROUP
    count = (last - first) // group

    def step(i, carry):
        for j in range(group):
            body(first + group * i + j)
        return carry

    lax.fori_loop(0, count, step, 0)
    for x in range(first + group * count, last):
        body(x)


def x_faces(force_ref, inv_ref, up_ref, low_ref, to_low_ref, to_up_ref):
    for which, ref in ((0, force_ref), (1, inv_ref)):
        for out, first in ((to_low_ref, 0), (to_up_ref, CX - W)):
            for t in range(T):
                for p in range(W):
                    x = first + p
                    out[which, t, EY * p : EY * p + CY, :] = ref[t, CY * x : CY * x + CY, :]
                    out[which, t, EY * p + CY : EY * p + EY, :] = jnp.zeros((8, 128), jnp.float32)
                    for r in range(W):
                        at = EY * p + CY + r
                        out[which, t, at : at + 1, :] = up_ref[which, r, t, x : x + 1, :]
                        at = EY * p + EY - W + r
                        out[which, t, at : at + 1, :] = low_ref[which, r, t, x : x + 1, :]


def assemble(force_ref, inv_ref, yup_ref, ylow_ref, xup_ref, xlow_ref, f_ref, v_ref, to_low_ref, to_up_ref):
    for which, (src, dst) in enumerate(((force_ref, f_ref), (inv_ref, v_ref))):
        for t in range(T):
            dst[t, 0 : EY * W, :] = xlow_ref[which, t]
            dst[t, EY * (W + CX) :, :] = xup_ref[which, t]
            for x in range(CX):
                at = EY * (W + x)
                dst[t, at : at + CY, :] = src[t, CY * x : CY * x + CY, :]
            at = EY * W + CY
            for r in range(W):
                dst[t, pl.ds(at + r, CX, EY), :] = yup_ref[which, r, t]
                dst[t, pl.ds(at + 8 - W + r, CX, EY), :] = ylow_ref[which, r, t]
            for r in range(W, 8 - W):
                dst[t, pl.ds(at + r, CX, EY), :] = jnp.zeros((CX, 128), jnp.float32)
    spot = lanes((128, 128))
    for j in range(ZB):
        first = min(128 * j, EX * EY - 128)
        at = slice(first, first + 128)
        mixed = jnp.where(
            spot < 16,
            f_ref[0, at, :],
            jnp.where(
                spot < 32,
                pltpu.roll(v_ref[0, at, :], 16, 1),
                jnp.where(spot < 48, pltpu.roll(f_ref[T - 1, at, :], 48, 1), pltpu.roll(v_ref[T - 1, at, :], 64, 1)),
            ),
        )
        turned = mixed.T
        to_low_ref[:, 128 * j : 128 * j + 128] = turned[0:32]
        to_up_ref[:, 128 * j : 128 * j + 128] = turned[32:64]


def smooth_kernel(_fin_ref, _vin_ref, zup_ref, zlow_ref, f_ref, v_ref, a_ref, to_low_ref, to_up_ref, coarse_ref, b_ref, tmp_ref):
    gap = jnp.zeros((96, 128), jnp.float32)
    for j in range(ZB):
        first = min(128 * j, EX * EY - 128)
        at = slice(128 * j, 128 * j + 128)
        for dst, part in ((f_ref, slice(0, 16)), (v_ref, slice(16, 32))):
            stack = jnp.concatenate([zup_ref[part, at], gap, zlow_ref[part, at]], axis=0)
            dst[T, first : first + 128, :] = stack.T

    def start(x):
        put_plane(a_ref, x, get(v_ref, x, EY) * get(f_ref, x, EY) * SCALE)

    planes(0, EX, start)
    (a1, b1), (a2, b2) = factors(3)

    def second(x):
        plane, beside = neighbours(a_ref, x, EY, 1)
        left = get(v_ref, x, EY) * (get(f_ref, x, EY) + beside) - plane
        put_plane(b_ref, x, (1.0 + a1) * plane + b1 * left)

    planes(1, EX - 1, second)

    def third(x):
        plane, beside = neighbours(b_ref, x, EY, 1)
        left = get(v_ref, x, EY) * (get(f_ref, x, EY) + beside) - plane
        put_plane(a_ref, x, plane + a2 * (plane - get(a_ref, x, EY)) + b2 * left)

    planes(2, EX - 2, third)
    even = lanes((CY // 2, EZ)) % 2 == 0

    def restrict(xc):
        total, weight = [], []
        for half in range(2):
            x = W + 2 * xc + half
            plane, beside = neighbours(a_ref, x, EY, 1)
            inv = get(v_ref, x, EY)[0:CY]
            diag = jnp.where(inv > 0.0, 1.0 / inv, 0.0)
            total.append((get(f_ref, x, EY) + beside)[0:CY] - diag * plane[0:CY])
            weight.append(diag)

        def pairs(value, slot):
            value = value + pltpu.roll(value, EZ - 1, 1)
            parts = []
            for t in range(TE):
                tmp_ref[slot, t] = value[:, 128 * t : 128 * t + 128]
                parts.append(tmp_ref[slot, t, pl.ds(0, CY // 2, 2)] + tmp_ref[slot, t, pl.ds(1, CY // 2, 2)])
            return jnp.concatenate(parts, axis=1)

        rhs = 0.5 * pairs(total[0] + total[1], 0)
        whole = pairs(weight[0] + weight[1], 1)
        inv = jnp.where(whole > 0.0, 1.0 / (6.0 + 0.5 * (whole - 48.0)), 0.0)
        put_plane(coarse_ref, xc, jnp.where(even, rhs, pltpu.roll(inv, 1, 1)))

    planes(0, CX // 2, restrict, 1)
    for t in range(TE):
        for r in range(WC):
            at = 8 * (r * TE + t)
            to_low_ref[at : at + 8, :] = coarse_ref[t, pl.ds(r, CX // 2, CY // 2), :]
            to_up_ref[at : at + 8, :] = coarse_ref[t, pl.ds(CY // 2 - WC + r, CX // 2, CY // 2), :]
        for r in range(W):
            at = 8 * WC * TE + 16 * (r * TE + t)
            to_low_ref[at : at + 16, :] = a_ref[t, pl.ds(EY * W + r, CX, EY), :]
            to_up_ref[at : at + 16, :] = a_ref[t, pl.ds(EY * W + CY - W + r, CX, EY), :]


def coarse_faces(own_ref, a_ref, up_ref, low_ref, to_low_ref, to_up_ref):
    none = jnp.zeros((8, 128), jnp.float32)
    for t in range(TE):
        for out, first in ((to_low_ref, 0), (to_up_ref, CX // 2 - WC)):
            for p in range(WC):
                x = first + p
                out[t, KY * p : KY * p + 16, :] = own_ref[t, 16 * x : 16 * x + 16, :]
                out[t, KY * p + 16 : KY * p + 24, :] = none
                out[t, KY * p + 24 : KY * p + 32, :] = none
            for r in range(WC):
                at = 8 * (r * TE + t) + first
                out[t, pl.ds(16 + r, WC, KY), :] = up_ref[at : at + WC, :]
                out[t, pl.ds(KY - WC + r, WC, KY), :] = low_ref[at : at + WC, :]
        base = KY * WC
        for out, first in ((to_low_ref, 0), (to_up_ref, CX - W)):
            for p in range(W):
                at, x = base + EY * p, EY * (W + first + p)
                out[t, at : at + CY, :] = a_ref[t, x : x + CY, :]
                out[t, at + CY : at + EY, :] = none
            for r in range(W):
                at = 8 * WC * TE + 16 * (r * TE + t) + first
                out[t, pl.ds(base + CY + r, W, EY), :] = up_ref[at : at + W, :]
                out[t, pl.ds(base + EY - W + r, W, EY), :] = low_ref[at : at + W, :]


def final_kernel(f_ref, v_ref, ain_ref, own_ref, yup_ref, ylow_ref, xup_ref, xlow_ref, out_ref, a_ref, b_ref, cb_ref, cv_ref, ca_ref, cc_ref, tmp_ref, res_ref, sems):
    half = CX // 2
    base = KY * WC
    for t in range(TE):
        cc_ref[t, 0:base, :] = xlow_ref[t, 0:base, :]
        cc_ref[t, KY * (WC + half) :, :] = xup_ref[t, 0:base, :]
        a_ref[t, 0 : EY * W, :] = xlow_ref[t, base:, :]
        a_ref[t, EY * (W + CX) :, :] = xup_ref[t, base:, :]
        for x in range(half):
            at = KY * (WC + x)
            cc_ref[t, at : at + 16, :] = own_ref[t, 16 * x : 16 * x + 16, :]
        at = KY * WC + 16
        for r in range(WC):
            src = slice(8 * (r * TE + t), 8 * (r * TE + t) + 8)
            cc_ref[t, pl.ds(at + r, half, KY), :] = yup_ref[src, :]
            cc_ref[t, pl.ds(at + 16 - WC + r, half, KY), :] = ylow_ref[src, :]
        for r in range(WC, 16 - WC):
            cc_ref[t, pl.ds(at + r, half, KY), :] = jnp.zeros((half, 128), jnp.float32)
        at = EY * W + CY
        for r in range(W):
            first = 8 * WC * TE + 16 * (r * TE + t)
            a_ref[t, pl.ds(at + r, CX, EY), :] = yup_ref[first : first + 16, :]
            a_ref[t, pl.ds(at + 8 - W + r, CX, EY), :] = ylow_ref[first : first + 16, :]
        for r in range(W, 8 - W):
            a_ref[t, pl.ds(at + r, CX, EY), :] = jnp.zeros((CX, 128), jnp.float32)
    even = lanes((KY, EZ)) % 2 == 0
    (a1, b1), (a2, b2), (a3, b3) = factors(4)

    def start(x):
        both = get(cc_ref, x, KY)
        right = jnp.where(even, both, pltpu.roll(both, 1, 1))
        inv = jnp.where(even, pltpu.roll(both, EZ - 1, 1), both)
        put_plane(cb_ref, x, right)
        put_plane(cv_ref, x, inv)
        put_plane(ca_ref, x, inv * right * SCALE)

    planes(0, KX, start)

    def sweep(src, dst, first, last, a, b, fresh):
        def body(x):
            plane, beside = neighbours(src, x, KY, 2)
            left = get(cv_ref, x, KY) * (get(cb_ref, x, KY) + beside) - plane
            step = plane if fresh else plane - get(dst, x, KY)
            put_plane(dst, x, plane + a * step + b * left)

        planes(first, last, body)

    sweep(ca_ref, cc_ref, 1, KX - 1, a1, b1, True)
    sweep(cc_ref, ca_ref, 2, KX - 2, a2, b2, False)
    sweep(ca_ref, cc_ref, 3, KX - 3, a3, b3, False)
    low = rows((8, 128)) < 4

    def spread(x, src):
        xc = (x - W + 2 * WC) // 2
        for t in range(TE):
            coarse = cc_ref[t, span(xc, KY), :]
            tmp_ref[t, pl.ds(0, 32, 2)] = coarse
            tmp_ref[t, pl.ds(1, 32, 2)] = coarse
            at = EY * x
            own, rim = pl.ds(pl.multiple_of(at, 8), CY), pl.ds(pl.multiple_of(at + CY, 8), 8)
            a_ref[t, own, :] = src[t, own, :] + tmp_ref[t, 0:CY]
            a_ref[t, rim, :] = a_ref[t, rim, :] + jnp.where(low, tmp_ref[t, 32:40], tmp_ref[t, 56:64])

    planes(0, W, lambda x: spread(x, a_ref), 1)
    planes(W, W + CX, lambda x: spread(x, ain_ref), 1)
    planes(W + CX, EX, lambda x: spread(x, a_ref), 1)
    (a1, b1), (a2, b2) = factors(3)

    def first(x):
        plane, beside = neighbours(a_ref, x, EY, 1)
        left = get(v_ref, x, EY) * (get(f_ref, x, EY) + beside) - plane
        put_plane(b_ref, x, plane + SCALE * left)

    planes(1, EX - 1, first)

    def second(x):
        plane, beside = neighbours(b_ref, x, EY, 1)
        left = get(v_ref, x, EY) * (get(f_ref, x, EY) + beside) - plane
        put_plane(a_ref, x, plane + a1 * (plane - get(a_ref, x, EY)) + b1 * left)

    planes(2, EX - 2, second)

    def third(x):
        plane, beside = neighbours(a_ref, x, EY, 1)
        left = get(v_ref, x, EY) * (get(f_ref, x, EY) + beside) - plane
        full = plane + a2 * (plane - get(b_ref, x, EY)) + b2 * left
        res_ref[x - W] = full[0:CY, 0:CZ]

    copies = []
    for i in range(4):
        at = pl.ds(4 * i, 4)
        planes(W + 4 * i, W + 4 * i + 4, third)
        copies.append(pltpu.make_async_copy(res_ref.at[at], out_ref.at[at], sems.at[i]))
        copies[-1].start()
    for copy in copies:
        copy.wait()


def swap(low, high, axis):
    count = lax.axis_size(axis)
    up = [(i, i + 1) for i in range(count - 1)]
    return lax.ppermute(low, axis, [(b, a) for a, b in up]), lax.ppermute(high, axis, up)


def solve(forcing, inverse, to_low, to_up):
    yup, ylow = swap(to_low, to_up, "gy")
    face = (2, T, W * EY, 128)
    xs = call(x_faces, [face, face], (forcing, inverse, yup, ylow), name="x_faces")
    xup, xlow = swap(*xs, "gx")
    ext = (TE, EX * EY, 128)
    f, v, zl, zu = call(
        assemble,
        [ext, ext, (32, 128 * ZB), (32, 128 * ZB)],
        (forcing, inverse, yup, ylow, xup, xlow),
        name="assemble",
    )
    zup, zlow = swap(zl, zu, "gz")
    cy, cx = (8 * TE * (WC + 2 * W), 128), (TE, KY * WC + EY * W, 128)
    f, v, a, yl, yu, own = call(
        smooth_kernel,
        [ext, ext, ext, cy, cy, (TE, CX // 2 * CY // 2, 128)],
        (f, v, zup, zlow),
        [pltpu.VMEM(ext, jnp.float32), pltpu.VMEM((2, TE, CY, 128), jnp.float32)],
        name="smooth",
        limit=8,
        alias={0: 0, 1: 1},
    )
    yup, ylow = swap(yl, yu, "gy")
    xs = call(coarse_faces, [cx, cx], (own, a, yup, ylow), name="coarse_faces")
    xup, xlow = swap(*xs, "gx")
    cext = pltpu.VMEM((TE, KX * KY, 128), jnp.float32)
    return call(
        final_kernel,
        [(CX, CY, CZ)],
        (f, v, a, own, yup, ylow, xup, xlow),
        [pltpu.VMEM(ext, jnp.float32)] * 2
        + [cext] * 4
        + [pltpu.VMEM((TE, 64, 128), jnp.float32), pltpu.VMEM((CX, CY, CZ), jnp.float32), pltpu.SemaphoreType.DMA((4,))],
        name="final",
        limit=20,
        far_out=(0,),
    )[0]


def bit_of(b, nv):
    if b < 3:
        return (lax.broadcasted_iota(jnp.int32, (8, 128), 0) >> b) & 1
    return (lax.broadcasted_iota(jnp.int32, (8, 128), 1) >> (b - 3 - nv)) & 1


def in_list(b, nv):
    return 3 <= b < 3 + nv


def across(x, b, nv, high):
    axis, size, d = (0, 8, 1 << b) if b < 3 else (1, 128, 1 << (b - 3 - nv))
    if 2 * d == size:
        return pltpu.roll(x, d, axis)
    return jnp.where(high, pltpu.roll(x, d, axis), pltpu.roll(x, size - d, axis))


def exchange(keys, values, b, nv):
    if in_list(b, nv):
        d = 1 << (b - 3)
        for u in range(len(keys)):
            if u & d:
                continue
            low, high = keys[u], keys[u + d]
            turn = low > high
            keys[u], keys[u + d] = jnp.minimum(low, high), jnp.maximum(low, high)
            a, c = values[u], values[u + d]
            values[u], values[u + d] = jnp.where(turn, c, a), jnp.where(turn, a, c)
        return
    high = bit_of(b, nv) != 0
    others = [across(key, b, nv, high) for key in keys]
    loads = [across(value, b, nv, high) for value in values]
    for u, other in enumerate(others):
        key = keys[u]
        keys[u] = jnp.where(high, jnp.maximum(key, other), jnp.minimum(key, other))
        values[u] = jnp.where(keys[u] != key, loads[u], values[u])


SIGN = -(1 << 31)


def route(goal, loads, b, nv, g):
    mask, one = jnp.int32(SIGN | (1 << g)), 1 << g
    if in_list(b, nv):
        d = 1 << (b - 3)
        for u in range(len(goal)):
            if u & d:
                continue
            low, high = goal[u], goal[u + d]
            ml, mh = low & mask, high & mask
            stay_l, stay_h = ml == 0, mh == one
            goal[u] = jnp.where(stay_l, low, jnp.where(mh == 0, high, -1))
            goal[u + d] = jnp.where(stay_h, high, jnp.where(ml == one, low, -1))
            for load in loads:
                a, c = load[u], load[u + d]
                load[u], load[u + d] = jnp.where(stay_l, a, c), jnp.where(stay_h, c, a)
        return
    place = bit_of(b, nv)
    high = place != 0
    place = place << g
    others = [across(x, b, nv, high) for x in goal]
    moved = [[across(x, b, nv, high) for x in load] for load in loads]
    for u, other in enumerate(others):
        own = goal[u]
        stay = (own & mask) == place
        goal[u] = jnp.where(stay, own, jnp.where((other & mask) == place, other, -1))
        for load, move in zip(loads, moved):
            load[u] = jnp.where(stay, load[u], move[u])


NONE = 1 << 18


def pack(owner_ref, cell_ref, jump_ref, turn, out_ref, key_ref, val_ref, goal_ref):
    nv = 3
    keys, values = [], []
    for u in range(8):
        at = slice(8 * u, 8 * u + 8)
        cell = cell_ref[at, :]
        mixed = (
            ((cell >> 15) << 15)
            | ((cell & 127) << 8)
            | ((cell >> 14) & 1) << 7
            | ((cell >> 12) & 3) << 5
            | ((cell >> 7) & 3) << 3
            | (cell >> 9) & 7
        )
        mixed = mixed ^ (turn * (NONE - 1))
        keys.append((owner_ref[at, :] << 18) | mixed)
        values.append(jump_ref[at, :])
    for k in range(1, 14):

        def flip(keys):
            if k == 13:
                return keys
            if in_list(k, nv):
                return [~key if (u >> (k - 3)) & 1 else key for u, key in enumerate(keys)]
            turned = -bit_of(k, nv)
            return [key ^ turned for key in keys]

        keys = flip(keys)
        for b in range(k - 1, -1, -1):
            exchange(keys, values, b, nv)
        keys = flip(keys)
    owners = [key >> 18 for key in keys]
    spot = 64 * lanes((8, 128)) + rows((8, 128))
    tail = [(owner << 13) | (8 * u + spot) for u, owner in enumerate(owners)]
    runs = list(tail)
    for b in range(13):
        if in_list(b, nv):
            d = 1 << (b - 3)
            other = [tail[u ^ d] for u in range(8)]
        else:
            d, high = 0, bit_of(b, nv) != 0
            other = [across(x, b, nv, high) for x in tail]
        for u in range(8):
            same = (other[u] ^ tail[u]) < 8192
            joins = (other[u] ^ runs[u]) < 8192
            if not d:
                runs[u] = jnp.where(high & joins, other[u], runs[u])
                tail[u] = jnp.where(high == same, other[u], tail[u])
            elif u & d:
                runs[u] = jnp.where(joins, other[u], runs[u])
                tail[u] = jnp.where(same, other[u], tail[u])
            else:
                tail[u] = jnp.where(same, tail[u], other[u])
    for u in range(8):
        at = slice(8 * u, 8 * u + 8)
        goal_ref[at, :] = 256 * owners[u] + 8 * u + spot - (runs[u] & 8191)
        key_ref[at, :] = (keys[u] & (NONE - 1)) ^ (turn * (NONE - 1))
        val_ref[at, :] = values[u]
    empty = NONE * (1 - turn) - turn

    def block(q, carry):
        sets = []
        for i in range(2):
            goal, key, value = [], [], []
            for u in range(8):
                at = slice(8 * u, 8 * u + 8)
                g = goal_ref[at, :]
                goal.append(jnp.where((g >> 13) == 2 * q + i, g & 8191, -1))
                key.append(key_ref[at, :])
                value.append(val_ref[at, :])
            sets.append((goal, key, value))
        for b in range(12, -1, -1):
            for goal, key, value in sets:
                route(goal, [key, value], b, nv, b)
        for i, (goal, key, value) in enumerate(sets):
            full = [g >= 0 for g in goal]
            parts = [jnp.where(f, v, 0.0) for f, v in zip(full, value)]
            parts += [jnp.where(f, c, empty).astype(jnp.float32) for f, c in zip(full, key)]
            first = pl.multiple_of(256 * q + 128 * i, 128)
            out_ref[pl.ds(first, 128), :] = jnp.concatenate(parts, axis=0).T
        return carry

    lax.fori_loop(0, 2, block, 0)


def regs(ref, first, count, step=8):
    return [ref[pl.ds(first + step * u, 8), :] for u in range(count)]


def put(ref, first, parts, step=8):
    for u, part in enumerate(parts):
        ref[pl.ds(first + step * u, 8), :] = part


def shifted(x, d):
    if d >= 256:
        return pltpu.roll(x, d // 256, 1)
    y = pltpu.roll(x, d, 0)
    head = max(d, 8)
    edge = jnp.where(rows((head, 128)) < d, pltpu.roll(y[:head], 1, 1), y[:head])
    return jnp.concatenate([edge, y[head:]], axis=0) if head < 256 else edge


def unpack_and_merge(got_ref, key_ref, val_ref):
    nv = 5
    for quarter in range(4):
        turned = got_ref[pl.ds(quarter, 128, 4), :].T
        val_ref[64 * quarter : 64 * quarter + 64, :] = turned[:64]
        key_ref[64 * quarter : 64 * quarter + 64, :] = turned[64:].astype(jnp.int32)
    before = 0
    for k in range(9, 16):
        turned = -bit_of(k, nv) if k < 15 else 0
        change = turned ^ before
        before = turned
        for b in range(k - 1, 7, -1):
            for half in range(2):
                keys, values = regs(key_ref, 128 * half, 16), regs(val_ref, 128 * half, 16)
                if b == k - 1:
                    keys = [key ^ change for key in keys]
                exchange(keys, values, b, nv)
                put(key_ref, 128 * half, keys)
                put(val_ref, 128 * half, values)
        for u in range(8):
            keys, values = regs(key_ref, 8 * u, 4, 64), regs(val_ref, 8 * u, 4, 64)
            for b in (4, 3):
                exchange(keys, values, b, 2)
            put(key_ref, 8 * u, keys, 64)
            put(val_ref, 8 * u, values, 64)
        for u in range(4):
            keys, values = regs(key_ref, 64 * u, 8), regs(val_ref, 64 * u, 8)
            for b in range(5, -1, -1):
                exchange(keys, values, b, 3)
            put(key_ref, 64 * u, keys)
            put(val_ref, 64 * u, values)


def combine(key_ref, val_ref, rank_ref):
    spot = rows((256, 128)) + 256 * lanes((256, 128))

    def gather(d):
        key, value = key_ref[...], val_ref[...]
        same = (shifted(key, d) == key) & (spot >= d)
        val_ref[...] = value + jnp.where(same, shifted(value, d), 0.0)

    for d in (1, 2, 4):
        gather(d)
    key = key_ref[...]
    real = (key >= 0) & (key < NONE)
    long = jnp.where(real & (shifted(key, 8) == key) & (spot >= 8), 1.0, 0.0)

    @pl.when(jnp.max(long) > 0.0)
    def _():
        for e in range(3, 15):
            gather(1 << e)

    after = pltpu.roll(key, 255, 0)
    edge = jnp.where(rows((8, 128)) == 7, pltpu.roll(after[248:], 127, 1), after[248:])
    after = jnp.concatenate([after[:248], edge], axis=0)
    last = real & ((after != key) | (spot == 32767))
    one = lambda test: jnp.where(test, 1.0, 0.0).astype(jnp.bfloat16)
    mask = one(last)
    dot = lambda a, b: jnp.dot(a, b, preferred_element_type=jnp.float32)
    within = dot(one(rows((256, 256)) > lanes((256, 256))), mask)
    totals = dot(jnp.ones((256, 256), jnp.bfloat16), mask).astype(jnp.bfloat16)
    before = dot(totals, one(rows((128, 128)) < lanes((128, 128))))
    rank_ref[...] = jnp.where(last, (within + before).astype(jnp.int32), -1)


def concentrate(key_ref, val_ref, rank_ref, turn_key_ref, turn_val_ref):
    refs = (rank_ref, key_ref, val_ref)

    def stages(first, count, step, bits):
        goal, key, value = (regs(r, first, count, step) for r in refs)
        for b, nv, g in bits:
            route(goal, [key, value], b, nv, g)
        for r, parts in zip(refs, (goal, key, value)):
            put(r, first, parts, step)

    for u in range(4):
        stages(64 * u, 8, 8, [(b, 3, b) for b in range(6)])
    for u in range(8):
        stages(8 * u, 4, 64, [(3, 2, 6), (4, 2, 7)])
    for b in range(8, 15):
        for half in range(2):
            stages(128 * half, 16, 8, [(b, 5, b)])
    for half in range(2):
        at = slice(128 * half, 128 * half + 128)
        turn_key_ref[at, :] = jnp.where(rank_ref[at, :] >= 0, key_ref[at, :], -1).T
        turn_val_ref[at, :] = val_ref[at, :].T


def distribute(turn_key_ref, turn_val_ref, goal_ref, move_ref, write):
    def block(q, carry):
        for half in range(2):
            goal, value = regs(turn_key_ref, 128 * half, 16), regs(turn_val_ref, 128 * half, 16)
            goal = [jnp.where((x >> 15) == q, x & 32767, -1) for x in goal]
            for b in range(6, -1, -1):
                route(goal, [value], b, 4, b + 8)
            at = slice(128 * half, 128 * half + 128)
            goal_ref[at, :] = jnp.concatenate(goal, axis=0).T
            move_ref[at, :] = jnp.concatenate(value, axis=0).T
        for u in range(8):
            goal, value = regs(goal_ref, 8 * u, 4, 64), regs(move_ref, 8 * u, 4, 64)
            route(goal, [value], 4, 2, 7)
            route(goal, [value], 3, 2, 6)
            put(goal_ref, 8 * u, goal, 64)
            put(move_ref, 8 * u, value, 64)
        for u in range(4):
            goal, value = regs(goal_ref, 64 * u, 8), regs(move_ref, 64 * u, 8)
            for b in range(5, -1, -1):
                route(goal, [value], b, 3, b)
            write(q, u, [jnp.where(x >= 0, v, 0.0) for x, v in zip(goal, value)])
        return carry

    lax.fori_loop(0, 8, block, 0)


def inverse_kernel(shift_hbm, inv_ref, to_low_ref, to_up_ref, shift_ref, sems):
    for i in range(2):
        at = pl.ds(i * (CX // 2), CX // 2)
        pltpu.make_async_copy(shift_hbm.at[at], shift_ref.at[at], sems.at[i]).start()
    for i in range(2):
        at = pl.ds(i * (CX // 2), CX // 2)
        pltpu.make_async_copy(shift_hbm.at[at], shift_ref.at[at], sems.at[i]).wait()

        def step(x, carry):
            for t in range(T):
                inv_ref[t, span(x, CY), :] = 1.0 / (6.0 + shift_ref[x, :, 128 * t : 128 * t + 128])
            return carry

        lax.fori_loop(i * (CX // 2), (i + 1) * (CX // 2), step, 0)
    for r in range(W):
        for t in range(T):
            to_low_ref[r, t] = inv_ref[t, pl.ds(r, CX, CY), :]
            to_up_ref[r, t] = inv_ref[t, pl.ds(CY - W + r, CX, CY), :]


def scatter_kernel(rhs_hbm, got_ref, inv_low_ref, inv_up_ref, force_ref, to_low_ref, to_up_ref, rhs_ref, key_ref, val_ref, rank_ref, turn_key_ref, turn_val_ref, sems):
    rhs_copy = pltpu.make_async_copy(rhs_hbm, rhs_ref, sems.at[0])
    rhs_copy.start()
    unpack_and_merge(got_ref, key_ref, val_ref)
    combine(key_ref, val_ref, rank_ref)
    concentrate(key_ref, val_ref, rank_ref, turn_key_ref, turn_val_ref)
    rhs_copy.wait()

    def write(q, u, values):
        x = 2 * q + u // 2
        for i, value in enumerate(values):
            row, t = 16 * (u % 2) + 8 * (i // 4), i % 4
            at = (x, slice(row, row + 8), slice(128 * t, 128 * t + 128))
            force_ref[t, pl.ds(pl.multiple_of(CY * x + row, 8), 8)] = rhs_ref[at] + value

    distribute(turn_key_ref, turn_val_ref, rank_ref, val_ref, write)
    to_low_ref[1] = inv_low_ref[...]
    to_up_ref[1] = inv_up_ref[...]
    for r in range(W):
        for t in range(T):
            to_low_ref[0, r, t] = force_ref[t, pl.ds(r, CX, CY), :]
            to_up_ref[0, r, t] = force_ref[t, pl.ds(CY - W + r, CX, CY), :]


def points_kernel(begin_ref, low_ref, up_ref, pos_hbm, nrm_hbm, ten_hbm, edge_hbm, conn_hbm, owner_hbm, cell_hbm, force_ref, send_ref, pos_ref, nrm_ref, ten_ref, edge_ref, conn_ref, owner_ref, cell_ref, jump_ref, key_ref, val_ref, goal_ref, sems):
    far = (pos_hbm, nrm_hbm, ten_hbm, edge_hbm, conn_hbm, owner_hbm, cell_hbm)
    near = (pos_ref, nrm_ref, ten_ref, edge_ref, conn_ref, owner_ref, cell_ref)
    copies = [pltpu.make_async_copy(a, b, sems.at[i]) for i, (a, b) in enumerate(zip(far, near))]
    for copy in copies:
        copy.start()
    for copy in copies:
        copy.wait()
    half = lanes((1, 128)) < 64
    tiles = NPOINT // 128

    def tile(ref, row, t):
        if t < 0:
            return low_ref[row : row + 1, :]
        if t >= tiles:
            return up_ref[row : row + 1, :]
        return ref[row : row + 1, 128 * t : 128 * t + 128]

    for t in range(tiles):
        at = slice(128 * t, 128 * t + 128)
        conn = conn_ref[:, at]
        edge = edge_ref[:, at]
        tension = ten_ref[t : t + 1, :]
        same = (conn >> 7) == begin_ref[0] + t
        spot = conn & 127
        jump = jnp.zeros((1, 128), jnp.float32)
        for c in range(3):
            own = tile(pos_ref, c, t)
            other = jnp.where(half, tile(pos_ref, c, t + 1), tile(pos_ref, c, t - 1))
            shape = conn.shape
            near = jnp.take_along_axis(jnp.broadcast_to(own, shape), spot, axis=1, mode="promise_in_bounds")
            far = jnp.take_along_axis(jnp.broadcast_to(other, shape), spot, axis=1, mode="promise_in_bounds")
            pull = jnp.sum(edge * (jnp.where(same, near, far) - own), axis=0, keepdims=True)
            force = tension * pull
            force_ref[c : c + 1, at] = force
            jump = jump + force * nrm_ref[c : c + 1, at]
        jump_ref[t : t + 1, :] = jump
    pack(owner_ref, cell_ref, jump_ref, begin_ref[1], send_ref, key_ref, val_ref, goal_ref)


def body(pressure_rhs, shift_diag, positions, normals, tension, edge_weight, owner_map, cell_map, connectivity):
    device = lax.axis_index(ALL)
    begin = jnp.stack([device * (NPOINT // 128), device % 2]).astype(jnp.int32)
    ring = [(i, (i + 1) % NDEV) for i in range(NDEV)]
    low = lax.ppermute(positions[:, NPOINT - 128 :], ALL, ring)
    up = lax.ppermute(positions[:, :128], ALL, [(b, a) for a, b in ring])
    flat = (NPOINT // 128, 128)
    whole = pltpu.VMEM(flat, jnp.int32)
    force, send = call(
        points_kernel,
        [(3, NPOINT), (4 * NDEV, 128)],
        (
            begin,
            low,
            up,
            positions,
            normals,
            tension.reshape(flat),
            edge_weight,
            connectivity,
            owner_map.reshape(flat),
            cell_map.reshape(flat),
        ),
        [pltpu.VMEM((3, NPOINT), jnp.float32)] * 2
        + [pltpu.VMEM(flat, jnp.float32), pltpu.VMEM((6, NPOINT), jnp.float32), pltpu.VMEM((6, NPOINT), jnp.int32)]
        + [whole, whole, pltpu.VMEM(flat, jnp.float32), whole, pltpu.VMEM(flat, jnp.float32), whole]
        + [pltpu.SemaphoreType.DMA((7,))],
        far=range(3, 10),
        name="points",
    )
    got = lax.all_to_all(send, ALL, 0, 0, tiled=True)
    block = pltpu.VMEM((CX, CY, CZ), jnp.float32)
    list_i, list_f = pltpu.VMEM((256, 128), jnp.int32), pltpu.VMEM((256, 128), jnp.float32)
    own, face = (T, CX * CY, 128), (2, W, T, CX, 128)
    inverse, inv_low, inv_up = call(
        inverse_kernel,
        [own, face[1:], face[1:]],
        (shift_diag,),
        [block, pltpu.SemaphoreType.DMA((2,))],
        name="inverse",
        far=(0,),
    )
    forcing, to_low, to_up = call(
        scatter_kernel,
        [own, face, face],
        (pressure_rhs, got, inv_low, inv_up),
        [block, list_i, list_f, list_i, list_i, list_f, pltpu.SemaphoreType.DMA((1,))],
        name="scatter",
        limit=8,
        far=(0,),
    )
    return solve(forcing, inverse, to_low, to_up), force


def solution(mesh):
    point, row = P(ALL), P(None, ALL)
    grid = P("gx", "gy", "gz")
    return jax.shard_map(
        body,
        mesh=mesh,
        in_specs=(grid, grid, row, row, point, row, P(ALL, None), point, row),
        out_specs=(grid, row),
        check_vma=False,
    )
```
